32 devices in a mesh: space: 4 (over y, x), sub: 8 (over z, core).
Axes of the slice: x: 2, y: 2, z: 4, core: 2. Of those that a mesh axis runs over, the one named last changes fastest.
Arguments:
- positions: float32 [3, 4, 512, 128], P(None, 'space', 'sub'), may hold values from 0 to 1.5
- masses: float32 [4, 512, 128], P('space', 'sub'), may hold values from 0.1 to 1
- occupancy: int32 [4, 512], P('space', 'sub'), may hold values from 1 to 128
- export_slots: int32 [4, 256], P('space', 'sub'), may hold values from 0 to 63, as said below
- export_count: int32 [4, 8], P('space', 'sub'), may hold values from 16 to 32
- pair_list: int32 [2, 4, 512], P(None, 'space', 'sub'), may hold values from 0 to 319, as said below
- pair_count: int32 [4, 8], P('space', 'sub'), may hold values from 16 to 64
Outputs:
- forces: float32 [3, 4, 512, 128], P(None, 'space', 'sub')
The draws below stay inside these ranges and needn't reach their ends.
Inputs may be any that keep to these rules, and one draw needn't show every extreme that they name: `export_slots`: the 32 entries of one device are distinct own-leaf indices. `pair_list`: row 0 is a target own leaf, below 64; row 1 is a source pool leaf, below 320, never equal to the target.
All inputs are finite; a program needn't handle non-finite values.
Results may differ from the reference program's by a relative error of at most 0.0003.
Values sent between devices are 32-bit elements; how exact they have to be, the bound alone decides.
No kernel may reach another device: no remote copies, remote signals or barrier semaphores. Data moves between devices by JAX's collectives and lax.ppermute only.
A program may use at most 64 MiB of HBM per device.

```python
import math
import jax
import jax.numpy as jnp
from jax import lax

LEAF = 128
LEAVES = 64
G = 32
PAIRS = 64
N_SPACE = 4
N_SUB = 8


def draw_export_slots(key, part):
    keys = jax.random.split(jax.random.fold_in(key, 7), N_SPACE * N_SUB)
    chosen = jax.vmap(lambda single: jax.random.permutation(single, LEAVES)[:G])(keys)
    return chosen.reshape(N_SPACE, N_SUB * G).astype(jnp.int32)


def draw_pair_list(key, part):
    first, second = jax.random.split(jax.random.fold_in(key, 11))
    targets = jax.random.randint(first, (N_SPACE, N_SUB * PAIRS), 0, LEAVES, dtype=jnp.int32)
    drawn = jax.random.randint(second, (N_SPACE, N_SUB * PAIRS), 0, LEAVES + 8 * G - 1, dtype=jnp.int32)
    sources = drawn + (drawn >= targets).astype(jnp.int32)
    return jnp.stack([targets, sources]).astype(jnp.int32)


def plant(values, stream_key, smallest, largest):
    spot = [jax.random.randint(jax.random.fold_in(stream_key, axis), (), 0, length) for axis, length in enumerate(values.shape)]
    longest = values.shape.index(max(values.shape))
    neighbour = spot[:longest] + [(spot[longest] + 1) % values.shape[longest]] + spot[longest + 1:]
    return values.at[tuple(spot)].set(smallest).at[tuple(neighbour)].set(largest)


def block_levels(stream_key, extent, cuts, least, high):
    level, own = 1.0, jax.random.fold_in(stream_key, 6)
    for position, shards_of in cuts:
        draws = jnp.exp(jax.random.uniform(jax.random.fold_in(own, position), (shards_of,), jnp.float32, least / len(cuts), high / len(cuts)))
        level = level * jnp.repeat(draws, extent[position] // shards_of).reshape([-1 if axis == position else 1 for axis in range(len(extent))])
    return level


def setup_inputs(seed: int = 0) -> dict:
    splits = jax.random.split(jax.random.key(seed), 8)
    positions = jnp.clip(1.5 * jax.random.uniform(splits[0], (3, N_SPACE, N_SUB * LEAVES, LEAF), jnp.float32) ** block_levels(splits[0], (3, N_SPACE, N_SUB * LEAVES, LEAF), ((1, 4), (2, 8)), -0.2, 0.2), 0.0, 1.5)
    masses = jnp.clip(jnp.exp(math.log(1.0) - 2.3025851 * jax.random.uniform(splits[1], (N_SPACE, N_SUB * LEAVES, LEAF), jnp.float32) ** block_levels(splits[1], (N_SPACE, N_SUB * LEAVES, LEAF), ((0, 4), (1, 8)), -0.2, 0.2)), 0.1, 1.0)
    occupancy = plant(jax.random.randint(splits[2], (N_SPACE, N_SUB * LEAVES), 1, LEAF + 1), jax.random.fold_in(splits[2], 1), 1, LEAF).astype(jnp.int32)
    export_slots = draw_export_slots(jax.random.fold_in(splits[7], 71), 0)
    export_count = plant(jax.random.randint(splits[4], (N_SPACE, N_SUB), G // 2, G + 1), jax.random.fold_in(splits[4], 1), G // 2, G).astype(jnp.int32)
    pair_list = draw_pair_list(jax.random.fold_in(splits[7], 71), 0)
    pair_count = plant(jax.random.randint(splits[6], (N_SPACE, N_SUB), PAIRS // 4, PAIRS + 1), jax.random.fold_in(splits[6], 1), PAIRS // 4, PAIRS).astype(jnp.int32)
    return dict(positions=positions, masses=masses, occupancy=occupancy, export_slots=export_slots, export_count=export_count, pair_list=pair_list, pair_count=pair_count)


OFFSETS = ((-1, -1), (-1, 0), (-1, 1), (0, -1), (0, 1), (1, -1), (1, 0), (1, 1))
SOFTEN = 0.05
PRECISE = lax.Precision.HIGHEST

def pair_block(target_pos, target_mass, source_pos, source_mass):
    separation = source_pos[:, :, None, :] - target_pos[:, :, :, None]
    distance = lax.optimization_barrier(jnp.sum(separation * separation, axis=0))
    falloff = jnp.maximum(1.0 - distance, 0.0)
    softened = distance + SOFTEN
    weight = target_mass[:, :, None] * source_mass[:, None, :] * falloff * falloff / (softened * jnp.sqrt(softened))
    row_total = lax.optimization_barrier(jnp.sum(weight, axis=2))
    col_total = lax.optimization_barrier(jnp.sum(weight, axis=1))
    on_target = jnp.einsum('bij,cbj->cbi', weight, source_pos, precision=PRECISE) - target_pos * row_total[None]
    on_source = jnp.einsum('bij,cbi->cbj', weight, target_pos, precision=PRECISE) - source_pos * col_total[None]
    return (on_target, on_source)

def device_forces(pool_pos, pool_mass, pair_rows, pair_total):
    own_index = jnp.arange(LEAVES, dtype=jnp.int32)
    live = (jnp.arange(PAIRS, dtype=jnp.int32) < pair_total).astype(jnp.float32)
    targets = jnp.concatenate([own_index, pair_rows[0]])
    sources = jnp.concatenate([own_index, pair_rows[1]])
    target_scale = jnp.concatenate([jnp.ones((LEAVES,), jnp.float32), live])
    source_scale = jnp.concatenate([jnp.zeros((LEAVES,), jnp.float32), live])

    def one_block(indices):
        tgt_rows, src_rows = indices
        return pair_block(pool_pos[:, tgt_rows], pool_mass[tgt_rows], pool_pos[:, src_rows], pool_mass[src_rows])
    on_target, on_source = lax.map(one_block, (targets.reshape(8, -1), sources.reshape(8, -1)))
    on_target = jnp.moveaxis(on_target, 0, 1).reshape(3, -1, LEAF)
    on_source = jnp.moveaxis(on_source, 0, 1).reshape(3, -1, LEAF)
    pool_force = jnp.zeros((3, pool_mass.shape[0], LEAF), jnp.float32)
    pool_force = pool_force.at[:, targets].add(on_target * target_scale[None, :, None])
    pool_force = pool_force.at[:, sources].add(on_source * source_scale[None, :, None])
    return pool_force

def reference(positions, masses, occupancy, export_slots, export_count, pair_list, pair_count):
    slot_index = lax.broadcasted_iota(jnp.int32, masses.shape, 2)
    live_mass = jnp.where(slot_index < occupancy[:, :, None], masses, 0.0)
    grid_pos = positions.reshape(3, N_SPACE, N_SUB, LEAVES, LEAF)
    grid_mass = live_mass.reshape(N_SPACE, N_SUB, LEAVES, LEAF)
    slots = export_slots.reshape(N_SPACE, N_SUB, G)
    keep = (jnp.arange(G, dtype=jnp.int32)[None, None, :] < export_count[:, :, None]).astype(jnp.float32)
    pos_index = jnp.broadcast_to(slots[None, :, :, :, None], (3, N_SPACE, N_SUB, G, LEAF))
    mass_index = jnp.broadcast_to(slots[:, :, :, None], (N_SPACE, N_SUB, G, LEAF))
    sent_pos = jnp.take_along_axis(grid_pos, pos_index, axis=3)
    sent_mass = jnp.take_along_axis(grid_mass, mass_index, axis=2) * keep[:, :, :, None]
    pos_list = [grid_pos]
    mass_list = [grid_mass]
    for space_step, sub_step in OFFSETS:
        pos_list.append(jnp.roll(sent_pos, (-space_step, -sub_step), axis=(1, 2)))
        mass_list.append(jnp.roll(sent_mass, (-space_step, -sub_step), axis=(0, 1)))
    pool_pos = jnp.concatenate(pos_list, axis=3)
    pool_mass = jnp.concatenate(mass_list, axis=2)
    pool_size = LEAVES + 8 * G
    device_total = N_SPACE * N_SUB
    dev_pos = jnp.moveaxis(pool_pos.reshape(3, device_total, pool_size, LEAF), 1, 0)
    dev_mass = pool_mass.reshape(device_total, pool_size, LEAF)
    dev_pairs = jnp.moveaxis(pair_list.reshape(2, device_total, PAIRS), 1, 0)
    dev_count = pair_count.reshape(device_total)

    def per_device(items):
        return device_forces(items[0], items[1], items[2], items[3])
    pool_force = lax.map(per_device, (dev_pos, dev_mass, dev_pairs, dev_count))
    pool_force = pool_force.reshape(N_SPACE, N_SUB, 3, pool_size, LEAF)
    own_force = pool_force[:, :, :, :LEAVES]
    returned = jnp.zeros((N_SPACE, N_SUB, 3, G, LEAF), jnp.float32)
    for order, (space_step, sub_step) in enumerate(OFFSETS):
        block = pool_force[:, :, :, LEAVES + order * G:LEAVES + (order + 1) * G]
        returned = returned + jnp.roll(block, (space_step, sub_step), axis=(0, 1))
    picker = (slots[:, :, :, None] == jnp.arange(LEAVES, dtype=jnp.int32)[None, None, None, :]).astype(jnp.float32)
    own_force = own_force + jnp.einsum('sbgl,sbcgp->sbclp', picker, returned, precision=PRECISE)
    forces = jnp.moveaxis(own_force, 2, 0)
    return forces.reshape(3, N_SPACE, N_SUB * LEAVES, LEAF)
```

```python
import functools

import jax
import jax.numpy as jnp
from jax import lax
from jax.experimental import pallas as pl
from jax.experimental.pallas import tpu as pltpu
from jax.sharding import PartitionSpec as P

OFFSETS = ((-1, -1), (-1, 0), (-1, 1), (0, -1), (0, 1), (1, -1), (1, 0), (1, 1))
LOCAL = 8
SOFTEN = 0.05
CENTER = 0.75
TABLE = 8
CODE = 1024
UNROLL = 4


def vmem():
    return pl.BlockSpec(memory_space=pltpu.VMEM)


def column(row, size):
    a = lax.broadcasted_iota(jnp.int32, (size, size), 0)
    b = lax.broadcasted_iota(jnp.int32, (size, size), 1)
    return jnp.sum(jnp.where(a == b, row[:, :size], 0), axis=1, keepdims=True)


def pack_kernel(pos, mass, occupancy, slots, count, pairs, pair_count, out, *, leaves, sent, slots_of_pairs):
    lanes = mass.shape[-1]
    occ = column(occupancy[...], leaves)
    lane = lax.broadcasted_iota(jnp.int32, (leaves, lanes), 1)
    live = jnp.where(lane < occ, mass[0], 0.0)
    for c in range(3):
        out[pl.ds(c, leaves, stride=4), :] = pos[c, 0] - CENTER
    out[pl.ds(3, leaves, stride=4), :] = live
    n = slots_of_pairs
    target = pairs[0]
    source = pairs[1]
    index = lax.broadcasted_iota(jnp.int32, (1, n), 1)
    key = jnp.where(source < leaves, LOCAL, (source - leaves) // sent)
    key = jnp.where(index < pair_count[0, 0], key, LOCAL + 1)
    code = target * CODE + source
    order = key * CODE + index
    order_col = column(order, n)
    code_col = column(code, n)
    rank = jnp.sum((order < order_col).astype(jnp.int32), axis=1, keepdims=True)
    place = lax.broadcasted_iota(jnp.int32, (n, lanes), 1)
    sorted_code = jnp.sum(jnp.where(place == rank, code_col, 0), axis=0, keepdims=True)
    starts = jnp.sum((order_col < place * CODE).astype(jnp.int32), axis=0, keepdims=True)
    g = lax.broadcasted_iota(jnp.int32, (1, sent), 1)
    alive = jnp.where(g < count[0, 0], slots[...], -1)
    base = 4 * leaves
    out[pl.ds(base, TABLE), :] = jnp.zeros((TABLE, lanes), jnp.float32)
    out[pl.ds(base, 1), :] = sorted_code.astype(jnp.float32)
    out[pl.ds(base + 1, 1), :] = starts.astype(jnp.float32)
    out[pl.ds(base + 2, 1), :sent] = alive.astype(jnp.float32)


def split3(a):
    a1 = a.astype(jnp.bfloat16).astype(jnp.float32)
    r = a - a1
    a2 = r.astype(jnp.bfloat16).astype(jnp.float32)
    return a1, a2, r - a2


def pair_force(target, source):
    row = lax.broadcasted_iota(jnp.int32, source.shape, 0)
    xs = jnp.where(row < 3, source, 0.0)
    xt = jnp.where(row < 3, target, 0.0)
    ms = source[3:4]
    qs = jnp.sum(xs * xs, axis=0, keepdims=True)
    qt = jnp.sum(xt * xt, axis=0, keepdims=True)
    a = jnp.where(row < 3, -2.0 * xs, jnp.where(row == 3, qs, jnp.where(row == 4, 1.0, 0.0)))
    b = jnp.where(row < 3, xt, jnp.where(row == 3, 1.0, jnp.where(row == 4, qt, 0.0)))
    a1, a2, a3 = split3(a)
    b1, b2, b3 = split3(b)
    left = jnp.concatenate([a1, a1, a2, a2, a1, a3], axis=0).astype(jnp.bfloat16)
    right = jnp.concatenate([b1, b2, b1, b2, b3, b1], axis=0).astype(jnp.bfloat16)
    distance = lax.dot_general(
        left, right, (((0,), (0,)), ((), ())), preferred_element_type=jnp.float32
    )
    inverse = lax.rsqrt(distance + SOFTEN)
    scaled = jnp.maximum(1.0 - distance, 0.0) * inverse
    weight = scaled * scaled * inverse
    high = weight.astype(jnp.bfloat16)
    low = (weight - high.astype(jnp.float32)).astype(jnp.bfloat16)
    g = jnp.where(row < 3, xs * ms, jnp.where(row == 3, ms, 0.0))
    g1, g2, g3 = split3(g)
    stack = jnp.concatenate([g1 + pltpu.roll(g2, 4, 0), g3], axis=0).astype(jnp.bfloat16)
    total = jnp.dot(stack, high, preferred_element_type=jnp.float32)
    total = total + jnp.dot(stack, low, preferred_element_type=jnp.float32)
    return total[:8] + total[8:]


def run_list(targets, sources, total, own, pool, acc):
    def step(i, carry):
        base = i * UNROLL
        outs = []
        for u in range(UNROLL):
            t = targets[base + u]
            s = sources[base + u]
            outs.append((t, pair_force(own[pl.ds(4 * t, 8), :], pool[pl.ds(s, 8), :])))
        for t, force in outs:
            at = pl.ds(pl.multiple_of(t * 8, 8), 8)
            acc[at, :] += force
        return carry

    lax.fori_loop(0, (total + UNROLL - 1) // UNROLL, step, 0)


def fetch_tables(packed, staging, tables, sem):
    for n, (ref, row) in enumerate(packed):
        staging[n] = ref[pl.ds(row, TABLE), :].astype(jnp.int32)
    copy = pltpu.make_async_copy(staging, tables, sem)
    copy.start()
    copy.wait()


def local_kernel(own, acc, staging, tables, targets, sources, sem, *, leaves):
    rows = 4 * leaves
    acc[...] = jnp.zeros_like(acc)
    fetch_tables([(own, rows)], staging, tables, sem)

    def itself(i, carry):
        targets[i] = i
        sources[i] = 4 * i
        return carry

    lax.fori_loop(0, leaves, itself, 0)

    def both(j, n):
        code = tables[0, 0, j]
        t = code // CODE
        u = code % CODE
        targets[n] = t
        sources[n] = 4 * u
        targets[n + 1] = u
        sources[n + 1] = 4 * t
        return n + 2

    total = lax.fori_loop(tables[0, 1, LOCAL], tables[0, 1, LOCAL + 1], both, leaves)
    for u in range(UNROLL):
        targets[total + u] = 0
        sources[total + u] = rows
    run_list(targets, sources, total, own, own, acc)


def ghost_list(tables, offsets, targets, sources, stride, leaves, sent):
    total = jnp.int32(0)
    for n, k in enumerate(offsets):
        row0 = n * stride

        def mine(j, total, n=n, k=k, row0=row0):
            code = tables[0, 0, j]
            leaf = tables[1 + n, 2, code % CODE - (leaves + k * sent)]
            targets[total] = code // CODE
            sources[total] = row0 + 4 * leaf
            return total + (leaf >= 0).astype(jnp.int32)

        total = lax.fori_loop(tables[0, 1, k], tables[0, 1, k + 1], mine, total)
        back = 7 - k

        def theirs(j, total, n=n, back=back, row0=row0):
            code = tables[1 + n, 0, j]
            leaf = tables[0, 2, code % CODE - (leaves + back * sent)]
            targets[total] = leaf
            sources[total] = row0 + 4 * (code // CODE)
            return total + (leaf >= 0).astype(jnp.int32)

        total = lax.fori_loop(tables[1 + n, 1, back], tables[1 + n, 1, back + 1], theirs, total)
    return total


def ghost_body(own, parts, acc_in, acc, pool, staging, tables, targets, sources, sem, offsets, leaves, sent):
    rows = 4 * leaves
    stride = rows + TABLE
    fetch_tables([(own, rows)] + [(ref, row + rows) for ref, row in parts], staging, tables, sem)
    for n, (ref, row) in enumerate(parts):
        pool[pl.ds(n * stride, stride), :] = ref[pl.ds(row, stride), :]
    total = ghost_list(tables, offsets, targets, sources, stride, leaves, sent)
    for u in range(UNROLL):
        targets[total + u] = 0
        sources[total + u] = rows
    run_list(targets, sources, total, own, pool, acc)


def face_kernel(own, p1, p3, p4, p6, acc_in, acc, pool, staging, tables, targets, sources, sem, *, leaves, sent):
    acc[...] = acc_in[...]
    parts = [(p1, 0), (p3, 0), (p4, 0), (p6, 0)]
    ghost_body(own, parts, acc_in, acc, pool, staging, tables, targets, sources, sem, (1, 3, 4, 6), leaves, sent)


def corner_kernel(own, lower, upper, acc_in, out, acc, pool, staging, tables, targets, sources, sem, *, leaves, sent):
    stride = 4 * leaves + TABLE
    acc[...] = acc_in[...]
    parts = [(lower, 0), (lower, stride), (upper, 0), (upper, stride)]
    ghost_body(own, parts, acc_in, acc, pool, staging, tables, targets, sources, sem, (0, 5, 2, 7), leaves, sent)

    def part(c):
        return acc[pl.ds(c, leaves, stride=8), :] + acc[pl.ds(c + 4, leaves, stride=8), :]

    mass = own[pl.ds(3, leaves, stride=4), :]
    norm = part(3)
    for c in range(3):
        out[c, 0] = mass * (part(c) - own[pl.ds(c, leaves, stride=4), :] * norm)


def ring(size, step):
    return [(i, (i + step) % size) for i in range(size)]


def both_ways(value, axis):
    size = lax.axis_size(axis)
    return (lax.ppermute(value, axis, ring(size, 1)), lax.ppermute(value, axis, ring(size, -1)))


def local(positions, masses, occupancy, export_slots, export_count, pair_list, pair_count):
    leaves, lanes = masses.shape[1:]
    sent = export_slots.shape[1]
    slots_of_pairs = pair_list.shape[2]
    rows = 4 * leaves + TABLE
    f32 = jnp.float32
    smem = pl.BlockSpec(memory_space=pltpu.SMEM)
    packed = pl.pallas_call(
        functools.partial(pack_kernel, leaves=leaves, sent=sent, slots_of_pairs=slots_of_pairs),
        out_shape=jax.ShapeDtypeStruct((rows, lanes), f32),
        in_specs=[vmem(), vmem(), vmem(), vmem(), smem, vmem(), smem],
        out_specs=vmem(),
        name="pack",
    )(positions, masses, occupancy, export_slots, export_count, pair_list, pair_count)

    def lists(tables, entries):
        return [
            pltpu.VMEM((tables, TABLE, lanes), jnp.int32),
            pltpu.SMEM((tables, TABLE, lanes), jnp.int32),
            pltpu.SMEM((entries + UNROLL,), jnp.int32),
            pltpu.SMEM((entries + UNROLL,), jnp.int32),
            pltpu.SemaphoreType.DMA,
        ]

    def cost(blocks):
        return pl.CostEstimate(flops=blocks * lanes * lanes * 200, transcendentals=0, bytes_accessed=rows * lanes * 4)

    accumulator = jax.ShapeDtypeStruct((8 * leaves, lanes), f32)
    lower_s, upper_s = both_ways(packed, "space")
    lower_r, upper_r = both_ways(packed, "sub")
    acc = pl.pallas_call(
        functools.partial(local_kernel, leaves=leaves),
        out_shape=accumulator,
        in_specs=[vmem()],
        out_specs=vmem(),
        scratch_shapes=lists(1, leaves + 2 * slots_of_pairs),
        cost_estimate=cost(leaves + slots_of_pairs),
        name="own",
    )(packed)
    corners = jnp.concatenate([lower_s, upper_s], axis=0)
    lower_c, upper_c = both_ways(corners, "sub")
    acc = pl.pallas_call(
        functools.partial(face_kernel, leaves=leaves, sent=sent),
        out_shape=accumulator,
        in_specs=[vmem()] * 6,
        out_specs=vmem(),
        scratch_shapes=[pltpu.VMEM((4 * rows, lanes), f32)] + lists(5, 5 * slots_of_pairs),
        cost_estimate=cost(slots_of_pairs),
        name="faces",
    )(packed, lower_s, lower_r, upper_r, upper_s, acc)
    return pl.pallas_call(
        functools.partial(corner_kernel, leaves=leaves, sent=sent),
        out_shape=jax.ShapeDtypeStruct((3, 1, leaves, lanes), f32),
        in_specs=[vmem()] * 4,
        out_specs=vmem(),
        scratch_shapes=[pltpu.VMEM((8 * leaves, lanes), f32), pltpu.VMEM((4 * rows, lanes), f32)]
        + lists(5, 5 * slots_of_pairs),
        cost_estimate=cost(slots_of_pairs),
        name="corners",
    )(packed, lower_c, upper_c, acc)


def solution(mesh):
    return jax.shard_map(
        local,
        mesh=mesh,
        in_specs=(
            P(None, "space", "sub", None),
            P("space", "sub", None),
            P("space", "sub"),
            P("space", "sub"),
            P("space", "sub"),
            P(None, "space", "sub"),
            P("space", "sub"),
        ),
        out_specs=P(None, "space", "sub", None),
        check_vma=False,
    )
```

```python
import functools

import jax
import jax.numpy as jnp
from jax import lax
from jax.experimental import pallas as pl
from jax.experimental.pallas import tpu as pltpu
from jax.sharding import PartitionSpec as P

OFFSETS = ((-1, -1), (-1, 0), (-1, 1), (0, -1), (0, 1), (1, -1), (1, 0), (1, 1))
LOCAL = 8
SOFTEN = 0.05
CENTER = 0.75
TABLE = 8
CODE = 1024
UNROLL = 8


def vmem():
    return pl.BlockSpec(memory_space=pltpu.VMEM)


def on_chip(value):
    return pltpu.with_memory_space_constraint(value, pltpu.VMEM)


def column(row, size):
    a = lax.broadcasted_iota(jnp.int32, (size, size), 0)
    b = lax.broadcasted_iota(jnp.int32, (size, size), 1)
    return jnp.sum(jnp.where(a == b, row[:, :size], 0), axis=1, keepdims=True)


def pack_kernel(pos, mass, occupancy, slots, count, pairs, pair_count, out, *, leaves, sent, slots_of_pairs):
    lanes = mass.shape[-1]
    occ = column(occupancy[...], leaves)
    lane = lax.broadcasted_iota(jnp.int32, (leaves, lanes), 1)
    live = jnp.where(lane < occ, mass[0], 0.0)
    for c in range(3):
        out[pl.ds(c, leaves, stride=4), :] = pos[c, 0] - CENTER
    out[pl.ds(3, leaves, stride=4), :] = live
    n = slots_of_pairs
    target = pairs[0]
    source = pairs[1]
    index = lax.broadcasted_iota(jnp.int32, (1, n), 1)
    key = jnp.where(source < leaves, LOCAL, (source - leaves) // sent)
    key = jnp.where(index < pair_count[0, 0], key, LOCAL + 1)
    code = target * CODE + source
    order = key * CODE + index
    order_col = column(order, n)
    code_col = column(code, n)
    rank = jnp.sum((order < order_col).astype(jnp.int32), axis=1, keepdims=True)
    place = lax.broadcasted_iota(jnp.int32, (n, lanes), 1)
    sorted_code = jnp.sum(jnp.where(place == rank, code_col, 0), axis=0, keepdims=True)
    starts = jnp.sum((order_col < place * CODE).astype(jnp.int32), axis=0, keepdims=True)
    g = lax.broadcasted_iota(jnp.int32, (1, sent), 1)
    alive = jnp.where(g < count[0, 0], slots[...], -1)
    base = 4 * leaves
    out[pl.ds(base, TABLE), :] = jnp.zeros((TABLE, lanes), jnp.float32)
    out[pl.ds(base, 1), :] = sorted_code.astype(jnp.float32)
    out[pl.ds(base + 1, 1), :] = starts.astype(jnp.float32)
    out[pl.ds(base + 2, 1), :sent] = alive.astype(jnp.float32)


def split3(a):
    a1 = a.astype(jnp.bfloat16).astype(jnp.float32)
    r = a - a1
    a2 = r.astype(jnp.bfloat16).astype(jnp.float32)
    return a1, a2, r - a2


def features(target, source):
    row = lax.broadcasted_iota(jnp.int32, source.shape, 0)
    xs = jnp.where(row < 3, source, 0.0)
    xt = jnp.where(row < 3, target, 0.0)
    ms = source[3:4]
    qs = jnp.sum(xs * xs, axis=0, keepdims=True) + SOFTEN
    qt = jnp.sum(xt * xt, axis=0, keepdims=True)
    a = jnp.where(row < 3, -2.0 * xs, jnp.where(row == 3, qs, jnp.where(row == 4, 1.0, 0.0)))
    b = jnp.where(row < 3, xt, jnp.where(row == 3, 1.0, jnp.where(row == 4, qt, 0.0)))
    g = jnp.where(row < 3, xs * ms, jnp.where(row == 3, ms, 0.0))
    a1, a2, a3 = split3(a)
    b1, b2, b3 = split3(b)
    g1, g2, g3 = split3(g)
    left = jnp.concatenate([a1, a1, a2, a2, a1, a3], axis=0).astype(jnp.bfloat16)
    right = jnp.concatenate([b1, b2, b1, b2, b3, b1], axis=0).astype(jnp.bfloat16)
    moments = jnp.concatenate([g1 + pltpu.roll(g2, 4, 0), g3], axis=0).astype(jnp.bfloat16)
    return left, right, moments


def moment_sums(softened, moments):
    inverse = lax.rsqrt(softened)
    scaled = jnp.maximum((1.0 + SOFTEN) - softened, 0.0) * inverse
    weight = scaled * scaled * inverse
    high = weight.astype(jnp.bfloat16)
    low = (weight - high.astype(jnp.float32)).astype(jnp.bfloat16)
    total = jnp.dot(moments, high, preferred_element_type=jnp.float32)
    total = total + jnp.dot(moments, low, preferred_element_type=jnp.float32)
    return total[:8] + total[8:]


def run_list(targets, sources, total, own, pool, acc, squares, weights):
    lanes = own.shape[1]
    squares[...] = jnp.full(squares.shape, 2.0, jnp.float32)
    weights[...] = jnp.zeros(weights.shape, jnp.bfloat16)

    def finish(base):
        sums = []
        for u in range(UNROLL):
            sums.append(moment_sums(squares[pl.ds(u * lanes, lanes), :], weights[pl.ds(16 * u, 16), :]))
        return sums

    def add(base, sums):
        for u in range(UNROLL):
            at = pl.ds(pl.multiple_of(targets[base + u] * 8, 8), 8)
            acc[at, :] += sums[u]

    def step(i, carry):
        base = i * UNROLL
        sums = finish(base)
        for u in range(UNROLL):
            t = targets[base + UNROLL + u]
            s = sources[base + UNROLL + u]
            left, right, moments = features(own[pl.ds(4 * t, 8), :], pool[pl.ds(s, 8), :])
            squares[pl.ds(u * lanes, lanes), :] = lax.dot_general(
                left, right, (((0,), (0,)), ((), ())), preferred_element_type=jnp.float32
            )
            weights[pl.ds(16 * u, 16), :] = moments
        add(base, sums)
        return carry

    steps = (total - 1) // UNROLL
    lax.fori_loop(0, steps, step, 0)
    add(steps * UNROLL, finish(steps * UNROLL))


def open_list(targets, sources, null_row):
    for u in range(UNROLL):
        targets[u] = 0
        sources[u] = null_row


def close_list(targets, sources, total, null_row):
    for u in range(UNROLL):
        targets[total + u] = 0
        sources[total + u] = null_row


def fetch_tables(packed, staging, tables, sem):
    for n, (ref, row) in enumerate(packed):
        staging[n] = ref[pl.ds(row, TABLE), :].astype(jnp.int32)
    copy = pltpu.make_async_copy(staging, tables, sem)
    copy.start()
    copy.wait()


def local_kernel(own, acc, staging, tables, targets, sources, squares, weights, sem, *, leaves):
    rows = 4 * leaves
    acc[...] = jnp.zeros_like(acc)
    fetch_tables([(own, rows)], staging, tables, sem)
    open_list(targets, sources, rows)

    def itself(i, carry):
        targets[UNROLL + i] = i
        sources[UNROLL + i] = 4 * i
        return carry

    lax.fori_loop(0, leaves, itself, 0)

    def both(j, n):
        code = tables[0, 0, j]
        t = code // CODE
        u = code % CODE
        targets[n] = t
        sources[n] = 4 * u
        targets[n + 1] = u
        sources[n + 1] = 4 * t
        return n + 2

    total = lax.fori_loop(tables[0, 1, LOCAL], tables[0, 1, LOCAL + 1], both, UNROLL + leaves)
    close_list(targets, sources, total, rows)
    run_list(targets, sources, total, own, own, acc, squares, weights)


def ghost_list(tables, offsets, targets, sources, stride, leaves, sent):
    total = jnp.int32(UNROLL)
    for n, k in enumerate(offsets):
        row0 = n * stride

        def mine(j, total, n=n, k=k, row0=row0):
            code = tables[0, 0, j]
            leaf = tables[1 + n, 2, code % CODE - (leaves + k * sent)]
            targets[total] = code // CODE
            sources[total] = row0 + 4 * leaf
            return total + (leaf >= 0).astype(jnp.int32)

        total = lax.fori_loop(tables[0, 1, k], tables[0, 1, k + 1], mine, total)
        back = 7 - k

        def theirs(j, total, n=n, back=back, row0=row0):
            code = tables[1 + n, 0, j]
            leaf = tables[0, 2, code % CODE - (leaves + back * sent)]
            targets[total] = leaf
            sources[total] = row0 + 4 * (code // CODE)
            return total + (leaf >= 0).astype(jnp.int32)

        total = lax.fori_loop(tables[1 + n, 1, back], tables[1 + n, 1, back + 1], theirs, total)
    return total


def ghost_body(own, parts, acc_in, acc, pool, staging, tables, targets, sources, squares, weights, sem, offsets, leaves, sent):
    rows = 4 * leaves
    stride = rows + TABLE
    fetch_tables([(own, rows)] + [(ref, row + rows) for ref, row in parts], staging, tables, sem)
    for n, (ref, row) in enumerate(parts):
        pool[pl.ds(n * stride, stride), :] = ref[pl.ds(row, stride), :]
    open_list(targets, sources, rows)
    total = ghost_list(tables, offsets, targets, sources, stride, leaves, sent)
    close_list(targets, sources, total, rows)
    run_list(targets, sources, total, own, pool, acc, squares, weights)


def face_kernel(own, p1, p3, p4, p6, acc_in, acc, pool, staging, tables, targets, sources, squares, weights, sem, *, leaves, sent):
    acc[...] = acc_in[...]
    parts = [(p1, 0), (p3, 0), (p4, 0), (p6, 0)]
    ghost_body(own, parts, acc_in, acc, pool, staging, tables, targets, sources, squares, weights, sem, (1, 3, 4, 6), leaves, sent)


def corner_kernel(own, lower, upper, acc_in, out, acc, pool, staging, tables, targets, sources, squares, weights, sem, *, leaves, sent):
    stride = 4 * leaves + TABLE
    acc[...] = acc_in[...]
    parts = [(lower, 0), (lower, stride), (upper, 0), (upper, stride)]
    ghost_body(own, parts, acc_in, acc, pool, staging, tables, targets, sources, squares, weights, sem, (0, 5, 2, 7), leaves, sent)

    def part(c):
        return acc[pl.ds(c, leaves, stride=8), :] + acc[pl.ds(c + 4, leaves, stride=8), :]

    mass = own[pl.ds(3, leaves, stride=4), :]
    norm = part(3)
    for c in range(3):
        out[c, 0] = mass * (part(c) - own[pl.ds(c, leaves, stride=4), :] * norm)


def ring(size, step):
    return [(i, (i + step) % size) for i in range(size)]


def both_ways(value, axis):
    size = lax.axis_size(axis)
    return (lax.ppermute(value, axis, ring(size, 1)), lax.ppermute(value, axis, ring(size, -1)))


def local(positions, masses, occupancy, export_slots, export_count, pair_list, pair_count):
    leaves, lanes = masses.shape[1:]
    sent = export_slots.shape[1]
    slots_of_pairs = pair_list.shape[2]
    rows = 4 * leaves + TABLE
    f32 = jnp.float32
    smem = pl.BlockSpec(memory_space=pltpu.SMEM)
    packed = pl.pallas_call(
        functools.partial(pack_kernel, leaves=leaves, sent=sent, slots_of_pairs=slots_of_pairs),
        out_shape=pltpu.VMEM((rows, lanes), f32),
        in_specs=[vmem(), vmem(), vmem(), vmem(), smem, vmem(), smem],
        out_specs=vmem(),
        name="pack",
    )(positions, masses, occupancy, export_slots, export_count, pair_list, pair_count)

    def lists(tables, entries):
        return [
            pltpu.VMEM((tables, TABLE, lanes), jnp.int32),
            pltpu.SMEM((tables, TABLE, lanes), jnp.int32),
            pltpu.SMEM((entries + 2 * UNROLL,), jnp.int32),
            pltpu.SMEM((entries + 2 * UNROLL,), jnp.int32),
            pltpu.VMEM((UNROLL * lanes, lanes), f32),
            pltpu.VMEM((UNROLL * 16, lanes), jnp.bfloat16),
            pltpu.SemaphoreType.DMA,
        ]

    def cost(blocks):
        return pl.CostEstimate(flops=blocks * lanes * lanes * 200, transcendentals=0, bytes_accessed=rows * lanes * 4)

    accumulator = pltpu.VMEM((8 * leaves, lanes), f32)
    lower_s, upper_s = both_ways(packed, "space")
    lower_r, upper_r = both_ways(packed, "sub")
    acc = pl.pallas_call(
        functools.partial(local_kernel, leaves=leaves),
        out_shape=accumulator,
        in_specs=[vmem()],
        out_specs=vmem(),
        scratch_shapes=lists(1, leaves + 2 * slots_of_pairs),
        cost_estimate=cost(leaves + slots_of_pairs),
        name="own",
    )(on_chip(packed))
    corners = jnp.concatenate([lower_s, upper_s], axis=0)
    lower_c, upper_c = both_ways(corners, "sub")
    acc = pl.pallas_call(
        functools.partial(face_kernel, leaves=leaves, sent=sent),
        out_shape=accumulator,
        in_specs=[vmem()] * 6,
        out_specs=vmem(),
        scratch_shapes=[pltpu.VMEM((4 * rows, lanes), f32)] + lists(5, 5 * slots_of_pairs),
        cost_estimate=cost(slots_of_pairs),
        name="faces",
    )(*map(on_chip, (packed, lower_s, lower_r, upper_r, upper_s, acc)))
    return pl.pallas_call(
        functools.partial(corner_kernel, leaves=leaves, sent=sent),
        out_shape=jax.ShapeDtypeStruct((3, 1, leaves, lanes), f32),
        in_specs=[vmem()] * 4,
        out_specs=vmem(),
        scratch_shapes=[pltpu.VMEM((8 * leaves, lanes), f32), pltpu.VMEM((4 * rows, lanes), f32)]
        + lists(5, 5 * slots_of_pairs),
        cost_estimate=cost(slots_of_pairs),
        name="corners",
    )(*map(on_chip, (packed, lower_c, upper_c, acc)))


def solution(mesh):
    return jax.shard_map(
        local,
        mesh=mesh,
        in_specs=(
            P(None, "space", "sub", None),
            P("space", "sub", None),
            P("space", "sub"),
            P("space", "sub"),
            P("space", "sub"),
            P(None, "space", "sub"),
            P("space", "sub"),
        ),
        out_specs=P(None, "space", "sub", None),
        check_vma=False,
    )
```

```python
import functools

import jax
import jax.numpy as jnp
from jax import lax
from jax.experimental import pallas as pl
from jax.experimental.pallas import tpu as pltpu
from jax.sharding import PartitionSpec as P


LOCAL = 8
SOFTEN = 0.05
CENTER = 0.75
TABLE = 8
CODE = 1024
BATCH = 8
CHUNK = 4


def vmem():
    return pl.BlockSpec(memory_space=pltpu.VMEM)


def on_chip(value):
    return pltpu.with_memory_space_constraint(value, pltpu.VMEM)


def column(row, size):
    a = lax.broadcasted_iota(jnp.int32, (size, size), 0)
    b = lax.broadcasted_iota(jnp.int32, (size, size), 1)
    return jnp.sum(jnp.where(a == b, row[:, :size], 0), axis=1, keepdims=True)


def pack_kernel(pos, mass, occupancy, slots, count, pairs, pair_count, out, *, leaves, sent, slots_of_pairs):
    lanes = mass.shape[-1]
    occ = column(occupancy[...], leaves)
    lane = lax.broadcasted_iota(jnp.int32, (leaves, lanes), 1)
    live = jnp.where(lane < occ, mass[0], 0.0)
    for c in range(3):
        out[pl.ds(c, leaves, stride=4), :] = pos[c, 0] - CENTER
    out[pl.ds(3, leaves, stride=4), :] = live
    n = slots_of_pairs
    target = pairs[0]
    source = pairs[1]
    index = lax.broadcasted_iota(jnp.int32, (1, n), 1)
    key = jnp.where(source < leaves, LOCAL, (source - leaves) // sent)
    key = jnp.where(index < pair_count[0, 0], key, LOCAL + 1)
    code = target * CODE + source
    order = key * CODE + index
    order_col = column(order, n)
    code_col = column(code, n)
    rank = jnp.sum((order < order_col).astype(jnp.int32), axis=1, keepdims=True)
    place = lax.broadcasted_iota(jnp.int32, (n, lanes), 1)
    sorted_code = jnp.sum(jnp.where(place == rank, code_col, 0), axis=0, keepdims=True)
    starts = jnp.sum((order_col < place * CODE).astype(jnp.int32), axis=0, keepdims=True)
    g = lax.broadcasted_iota(jnp.int32, (1, sent), 1)
    alive = jnp.where(g < count[0, 0], slots[...], -1)
    base = 4 * leaves
    out[pl.ds(base, TABLE), :] = jnp.zeros((TABLE, lanes), jnp.float32)
    out[pl.ds(base, 1), :] = sorted_code.astype(jnp.float32)
    out[pl.ds(base + 1, 1), :] = starts.astype(jnp.float32)
    out[pl.ds(base + 2, 1), :sent] = alive.astype(jnp.float32)


def split3(a):
    a1 = a.astype(jnp.bfloat16).astype(jnp.float32)
    r = a - a1
    a2 = r.astype(jnp.bfloat16).astype(jnp.float32)
    return a1, a2, r - a2


def features(target, source):
    row = lax.broadcasted_iota(jnp.int32, source.shape, 0)
    xs = jnp.where(row < 3, source, 0.0)
    xt = jnp.where(row < 3, target, 0.0)
    ms = source[3:4]
    qs = jnp.sum(xs * xs, axis=0, keepdims=True) + SOFTEN
    qt = jnp.sum(xt * xt, axis=0, keepdims=True)
    a = jnp.where(row < 3, -2.0 * xs, jnp.where(row == 3, qs, jnp.where(row == 4, 1.0, 0.0)))
    b = jnp.where(row < 3, xt, jnp.where(row == 3, 1.0, jnp.where(row == 4, qt, 0.0)))
    g = jnp.where(row < 3, xs * ms, jnp.where(row == 3, ms, 0.0))
    a1, a2, a3 = split3(a)
    b1, b2, b3 = split3(b)
    g1, g2, g3 = split3(g)
    left = jnp.concatenate([a1, a1, a2, a2, a1, a3], axis=0).astype(jnp.bfloat16)
    right = jnp.concatenate([b1, b2, b1, b2, b3, b1], axis=0).astype(jnp.bfloat16)
    moments = jnp.concatenate([g1 + pltpu.roll(g2, 4, 0), g3], axis=0).astype(jnp.bfloat16)
    return left, right, moments


def moment_sums(softened, moments):
    lanes = softened.shape[1] // 2
    inverse = lax.rsqrt(softened)
    scaled = jnp.maximum((1.0 + SOFTEN) - softened, 0.0) * inverse
    weight = scaled * scaled * inverse
    high = weight.astype(jnp.bfloat16)
    low = (weight - high.astype(jnp.float32)).astype(jnp.bfloat16)
    total = jnp.dot(
        jnp.concatenate([moments, moments], axis=1),
        jnp.concatenate([high, low], axis=0),
        preferred_element_type=jnp.float32,
    )
    return (
        total[0:8, :lanes] + total[8:16, :lanes],
        total[16:24, lanes:] + total[24:32, lanes:],
    )


def run_pairs(batches, first, second, own, pool, acc, squares, weights):
    lanes = own.shape[1]
    none = jnp.zeros((48, lanes), jnp.bfloat16)

    def begin(i):
        for u in range(0, BATCH, 2):
            sides = [
                features(own[pl.ds(4 * first(i, v), 8), :], pool[pl.ds(second(i, v), 8), :]) for v in (u, u + 1)
            ]
            left = jnp.concatenate([sides[0][0], sides[1][0]], axis=0)
            right = jnp.concatenate(
                [
                    jnp.concatenate([sides[0][1], none], axis=1),
                    jnp.concatenate([none, sides[1][1]], axis=1),
                ],
                axis=0,
            )
            squares[u // 2] = lax.dot_general(
                left, right, (((0,), (0,)), ((), ())), preferred_element_type=jnp.float32
            )
            weights[u // 2] = jnp.concatenate([sides[0][2], sides[1][2]], axis=0)

    def finish():
        return [force for unit in range(BATCH // 2) for force in moment_sums(squares[unit], weights[unit])]

    def add(i, sums):
        for u in range(BATCH):
            at = pl.ds(pl.multiple_of(first(i, u) * 8, 8), 8)
            acc[at, :] += sums[u]

    def step(i, carry):
        sums = finish()
        begin(i)
        add(i - 1, sums)
        return carry

    begin(0)
    lax.fori_loop(1, batches, step, 0)
    add(batches - 1, finish())


def run_list(targets, sources, total, null_row, own, pool, acc, squares, weights):
    for u in range(BATCH):
        targets[total + u] = 0
        sources[total + u] = null_row
    batches = jnp.maximum((total + BATCH - 1) // BATCH, 1)
    run_pairs(
        batches,
        lambda i, u: targets[i * BATCH + u],
        lambda i, u: sources[i * BATCH + u],
        own, pool, acc, squares, weights,
    )


def fetch_tables(packed, staging, tables, sem):
    for n, (ref, row) in enumerate(packed):
        staging[n] = ref[pl.ds(row, TABLE), :].astype(jnp.int32)
    copy = pltpu.make_async_copy(staging, tables, sem)
    copy.start()
    return copy


def append(begin, end, entry, targets, sources, total):
    def step(i, total):
        j = begin + i * CHUNK
        found = [entry(j + v) for v in range(CHUNK)]
        for v, (target, source, valid) in enumerate(found):
            targets[total] = target
            sources[total] = source
            total = total + jnp.where((j + v < end) & valid, 1, 0)
        return total

    return lax.fori_loop(0, lax.shift_right_logical(end - begin + (CHUNK - 1), CHUNK.bit_length() - 1), step, total)


def append_ghosts(tables, offsets, row0, stride, targets, sources, total, leaves, sent):
    lanes = tables.shape[2]
    bits = CODE.bit_length() - 1

    def slot(code, k):
        return ((code & (CODE - 1)) - (leaves + k * sent)) & (lanes - 1)

    for n, k in enumerate(offsets):
        at = row0 + n * stride

        def mine(j, n=n, k=k, at=at):
            code = tables[0, 0, j]
            leaf = tables[1 + n, 2, slot(code, k)]
            return lax.shift_right_logical(code, bits), at + 4 * leaf, leaf >= 0

        total = append(tables[0, 1, k], tables[0, 1, k + 1], mine, targets, sources, total)
        back = 7 - k

        def theirs(j, n=n, back=back, at=at):
            code = tables[1 + n, 0, j]
            leaf = tables[0, 2, slot(code, back)]
            return leaf, at + 4 * lax.shift_right_logical(code, bits), leaf >= 0

        total = append(tables[1 + n, 1, back], tables[1 + n, 1, back + 1], theirs, targets, sources, total)
    return total


def self_kernel(own, acc, squares, weights, *, leaves):
    acc[...] = jnp.zeros_like(acc)
    run_pairs(
        leaves // BATCH,
        lambda i, u: i * BATCH + u,
        lambda i, u: 4 * (i * BATCH + u),
        own, own, acc, squares, weights,
    )


def near_kernel(own, p1, p3, p4, p6, acc_in, acc, pool, staging, tables, targets, sources, squares, weights, sem, *, leaves, sent):
    rows = 4 * leaves
    stride = rows + TABLE
    parts = (own, p1, p3, p4, p6)
    copy = fetch_tables([(ref, rows) for ref in parts], staging, tables, sem)
    acc[...] = acc_in[...]
    for n, ref in enumerate(parts):
        pool[pl.ds(n * stride, stride), :] = ref[...]
    copy.wait()

    def both(j, n):
        code = tables[0, 0, j]
        t = lax.shift_right_logical(code, CODE.bit_length() - 1)
        u = code & (CODE - 1)
        targets[n] = t
        sources[n] = 4 * u
        targets[n + 1] = u
        sources[n + 1] = 4 * t
        return n + 2

    total = lax.fori_loop(tables[0, 1, LOCAL], tables[0, 1, LOCAL + 1], both, 0)
    total = append_ghosts(tables, (1, 3, 4, 6), stride, stride, targets, sources, total, leaves, sent)
    run_list(targets, sources, total, rows, own, pool, acc, squares, weights)


def corner_kernel(own, lower, upper, acc_in, out, acc, pool, staging, tables, targets, sources, squares, weights, sem, *, leaves, sent):
    rows = 4 * leaves
    stride = rows + TABLE
    parts = [(lower, 0), (lower, stride), (upper, 0), (upper, stride)]
    copy = fetch_tables([(own, rows)] + [(ref, row + rows) for ref, row in parts], staging, tables, sem)
    acc[...] = acc_in[...]
    pool[pl.ds(0, 2 * stride), :] = lower[...]
    pool[pl.ds(2 * stride, 2 * stride), :] = upper[...]
    copy.wait()
    total = append_ghosts(tables, (0, 5, 2, 7), 0, stride, targets, sources, 0, leaves, sent)
    run_list(targets, sources, total, rows, own, pool, acc, squares, weights)

    def part(c):
        return acc[pl.ds(c, leaves, stride=8), :] + acc[pl.ds(c + 4, leaves, stride=8), :]

    mass = own[pl.ds(3, leaves, stride=4), :]
    norm = part(3)
    for c in range(3):
        out[c, 0] = mass * (part(c) - own[pl.ds(c, leaves, stride=4), :] * norm)


def ring(size, step):
    return [(i, (i + step) % size) for i in range(size)]


def both_ways(value, axis):
    size = lax.axis_size(axis)
    lower = lax.ppermute(value, axis, ring(size, 1))
    upper = lax.ppermute(value, axis, ring(size, -1))
    return lower, upper


def local(positions, masses, occupancy, export_slots, export_count, pair_list, pair_count):
    leaves, lanes = masses.shape[1:]
    sent = export_slots.shape[1]
    slots_of_pairs = pair_list.shape[2]
    rows = 4 * leaves + TABLE
    f32 = jnp.float32
    smem = pl.BlockSpec(memory_space=pltpu.SMEM)
    packed = pl.pallas_call(
        functools.partial(pack_kernel, leaves=leaves, sent=sent, slots_of_pairs=slots_of_pairs),
        out_shape=pltpu.VMEM((rows, lanes), f32),
        in_specs=[vmem(), vmem(), vmem(), vmem(), smem, vmem(), smem],
        out_specs=vmem(),
        name="pack",
    )(positions, masses, occupancy, export_slots, export_count, pair_list, pair_count)

    pairing = [
        pltpu.VMEM((BATCH // 2, lanes, 2 * lanes), f32),
        pltpu.VMEM((BATCH // 2, 32, lanes), jnp.bfloat16),
    ]

    def lists(entries):
        return [
            pltpu.VMEM((5, TABLE, lanes), jnp.int32),
            pltpu.SMEM((5, TABLE, lanes), jnp.int32),
            pltpu.SMEM((entries + BATCH + CHUNK,), jnp.int32),
            pltpu.SMEM((entries + BATCH + CHUNK,), jnp.int32),
            *pairing,
            pltpu.SemaphoreType.DMA,
        ]

    def cost(blocks):
        return pl.CostEstimate(flops=blocks * lanes * lanes * 200, transcendentals=0, bytes_accessed=rows * lanes * 4)

    accumulator = pltpu.VMEM((8 * leaves, lanes), f32)
    lower_s, upper_s = both_ways(packed, "space")
    lower_r, upper_r = both_ways(packed, "sub")
    acc = pl.pallas_call(
        functools.partial(self_kernel, leaves=leaves),
        out_shape=accumulator,
        in_specs=[vmem()],
        out_specs=vmem(),
        scratch_shapes=pairing,
        cost_estimate=cost(leaves),
        name="self_pairs",
    )(on_chip(packed))
    corners = jnp.concatenate([lower_s, upper_s], axis=0)
    lower_c, upper_c = both_ways(corners, "sub")
    acc = pl.pallas_call(
        functools.partial(near_kernel, leaves=leaves, sent=sent),
        out_shape=accumulator,
        in_specs=[vmem()] * 6,
        out_specs=vmem(),
        scratch_shapes=[pltpu.VMEM((5 * rows, lanes), f32)] + lists(6 * slots_of_pairs),
        cost_estimate=cost(slots_of_pairs),
        name="near_pairs",
    )(*map(on_chip, (packed, lower_s, lower_r, upper_r, upper_s, acc)))
    return pl.pallas_call(
        functools.partial(corner_kernel, leaves=leaves, sent=sent),
        out_shape=jax.ShapeDtypeStruct((3, 1, leaves, lanes), f32),
        in_specs=[vmem()] * 4,
        out_specs=vmem(),
        scratch_shapes=[pltpu.VMEM((8 * leaves, lanes), f32), pltpu.VMEM((4 * rows, lanes), f32)]
        + lists(5 * slots_of_pairs),
        cost_estimate=cost(slots_of_pairs),
        name="corner_pairs",
    )(*map(on_chip, (packed, lower_c, upper_c, acc)))


def solution(mesh):
    return jax.shard_map(
        local,
        mesh=mesh,
        in_specs=(
            P(None, "space", "sub", None),
            P("space", "sub", None),
            P("space", "sub"),
            P("space", "sub"),
            P("space", "sub"),
            P(None, "space", "sub"),
            P("space", "sub"),
        ),
        out_specs=P(None, "space", "sub", None),
        check_vma=False,
    )
```

```python
import functools

import jax
import jax.numpy as jnp
from jax import lax
from jax.experimental import pallas as pl
from jax.experimental.pallas import tpu as pltpu
from jax.sharding import PartitionSpec as P


LOCAL = 8
SOFTEN = 0.05
CENTER = 0.75
TABLE = 8
CODE = 1024
SELF_BATCH, NEAR_BATCH, FAR_BATCH = 16, 8, 12
CHUNK = 4


def vmem():
    return pl.BlockSpec(memory_space=pltpu.VMEM)


def on_chip(value):
    return pltpu.with_memory_space_constraint(value, pltpu.VMEM)


def column(row, size):
    a = lax.broadcasted_iota(jnp.int32, (size, size), 0)
    b = lax.broadcasted_iota(jnp.int32, (size, size), 1)
    return jnp.sum(jnp.where(a == b, row[:, :size], 0), axis=1, keepdims=True)


def pack_kernel(pos, mass, occupancy, slots, pairs, counts, out, *, leaves, sent, slots_of_pairs):
    lanes = mass.shape[-1]
    occ = column(occupancy[...], leaves)
    lane = lax.broadcasted_iota(jnp.int32, (leaves, lanes), 1)
    live = jnp.where(lane < occ, mass[0], 0.0)
    for c in range(3):
        out[pl.ds(c, leaves, stride=4), :] = pos[c, 0] - CENTER
    out[pl.ds(3, leaves, stride=4), :] = live
    n = slots_of_pairs
    target = pairs[0]
    source = pairs[1]
    index = lax.broadcasted_iota(jnp.int32, (1, n), 1)
    key = jnp.where(source < leaves, LOCAL, (source - leaves) // sent)
    key = jnp.where(index < counts[:, lanes // 2 : lanes // 2 + 1], key, LOCAL + 1)
    code = target * CODE + source
    order = key * CODE + index
    order_col = column(order, n)
    code_col = column(code, n)
    rank = jnp.sum((order < order_col).astype(jnp.int32), axis=1, keepdims=True)
    place = lax.broadcasted_iota(jnp.int32, (n, lanes), 1)
    sorted_code = jnp.sum(jnp.where(place == rank, code_col, 0), axis=0, keepdims=True)
    starts = jnp.sum((order_col < place * CODE).astype(jnp.int32), axis=0, keepdims=True)
    g = lax.broadcasted_iota(jnp.int32, (1, sent), 1)
    alive = jnp.where(g < counts[:, 0:1], slots[...], -1)
    base = 4 * leaves
    out[pl.ds(base, TABLE), :] = jnp.zeros((TABLE, lanes), jnp.float32)
    out[pl.ds(base, 1), :] = sorted_code.astype(jnp.float32)
    out[pl.ds(base + 1, 1), :] = starts.astype(jnp.float32)
    out[pl.ds(base + 2, 1), :sent] = alive.astype(jnp.float32)


def split3(a):
    a1 = a.astype(jnp.bfloat16).astype(jnp.float32)
    r = a - a1
    a2 = r.astype(jnp.bfloat16).astype(jnp.float32)
    return a1, a2, r - a2


STACK = 48


def target_stack(target):
    row = lax.broadcasted_iota(jnp.int32, target.shape, 0)
    xt = jnp.where(row < 3, target, 0.0)
    qt = jnp.sum(xt * xt, axis=0, keepdims=True)
    b = jnp.where(row < 3, xt, jnp.where(row == 3, 1.0, jnp.where(row == 4, qt, 0.0)))
    b1, b2, b3 = split3(b)
    return jnp.concatenate([b1, b2, b1, b2, b3, b1], axis=0).astype(jnp.bfloat16)


def source_stacks(source):
    row = lax.broadcasted_iota(jnp.int32, source.shape, 0)
    xs = jnp.where(row < 3, source, 0.0)
    ms = source[3:4]
    qs = jnp.sum(xs * xs, axis=0, keepdims=True) + SOFTEN
    a = jnp.where(row < 3, -2.0 * xs, jnp.where(row == 3, qs, jnp.where(row == 4, 1.0, 0.0)))
    g = jnp.where(row < 3, xs * ms, jnp.where(row == 3, ms, 0.0))
    a1, a2, a3 = split3(a)
    g1, g2, g3 = split3(g)
    left = jnp.concatenate([a1, a1, a2, a2, a1, a3], axis=0).astype(jnp.bfloat16)
    moments = jnp.concatenate([g1 + pltpu.roll(g2, 4, 0), g3], axis=0).astype(jnp.bfloat16)
    return left, moments


def moment_sums(softened, moments):
    lanes = softened.shape[1] // 2
    inverse = lax.rsqrt(softened)
    scaled = jnp.maximum((1.0 + SOFTEN) - softened, 0.0) * inverse
    weight = scaled * scaled * inverse
    high = weight.astype(jnp.bfloat16)
    low = (weight - high.astype(jnp.float32)).astype(jnp.bfloat16)
    total = jnp.dot(
        jnp.concatenate([moments, moments], axis=1),
        jnp.concatenate([high, low], axis=0),
        preferred_element_type=jnp.float32,
    )
    return (
        total[0:8, :lanes] + total[8:16, :lanes],
        total[16:24, lanes:] + total[24:32, lanes:],
    )


def run_pairs(batches, first, second, target_of, pool, acc, squares, weights):
    lanes = pool.shape[1]
    size = 2 * squares.shape[0]
    none = jnp.zeros((STACK, lanes), jnp.bfloat16)

    def begin(i):
        begun = []
        for u in range(0, size, 2):
            rights = [target_of(first(i, v)) for v in (u, u + 1)]
            lefts = [source_stacks(pool[pl.ds(second(i, v), 8), :]) for v in (u, u + 1)]
            left = jnp.concatenate([lefts[0][0], lefts[1][0]], axis=0)
            right = jnp.concatenate(
                [
                    jnp.concatenate([rights[0], none], axis=1),
                    jnp.concatenate([none, rights[1]], axis=1),
                ],
                axis=0,
            )
            square = lax.dot_general(left, right, (((0,), (0,)), ((), ())), preferred_element_type=jnp.float32)
            begun.append((square, jnp.concatenate([lefts[0][1], lefts[1][1]], axis=0)))
        return begun

    def keep(begun):
        for unit, (square, moments) in enumerate(begun):
            squares[unit] = square
            weights[unit] = moments

    def finish():
        return [force for unit in range(size // 2) for force in moment_sums(squares[unit], weights[unit])]

    def add(i, sums):
        for u in range(size):
            at = pl.ds(pl.multiple_of(first(i, u) * 8, 8), 8)
            acc[at, :] += sums[u]

    def step(i, carry):
        begun = begin(i)
        sums = finish()
        keep(begun)
        add(i - 1, sums)
        return carry

    keep(begin(0))
    lax.fori_loop(1, batches, step, 0)
    add(batches - 1, finish())


def run_list(targets, sources, total, null_row, stacks, pool, acc, squares, weights):
    size = 2 * squares.shape[0]
    for u in range(size):
        targets[total + u] = 0
        sources[total + u] = null_row
    batches = jnp.maximum(lax.div(total + (size - 1), size), 1)
    run_pairs(
        batches,
        lambda i, u: targets[i * size + u],
        lambda i, u: sources[i * size + u],
        lambda leaf: stacks[leaf],
        pool, acc, squares, weights,
    )


def append(begin, end, entry, targets, sources, total):
    def step(i, total):
        j = begin + i * CHUNK
        found = [entry(j + v) for v in range(CHUNK)]
        for v, (target, source, valid) in enumerate(found):
            targets[total] = target
            sources[total] = source
            total = total + jnp.where((j + v < end) & valid, 1, 0)
        return total

    return lax.fori_loop(0, lax.shift_right_logical(end - begin + (CHUNK - 1), CHUNK.bit_length() - 1), step, total)


def append_ghosts(tables, offsets, first, stride, targets, sources, total, leaves, sent):
    lanes = tables.shape[2]
    bits = CODE.bit_length() - 1

    def slot(code, k):
        return ((code & (CODE - 1)) - (leaves + k * sent)) & (lanes - 1)

    for n, k in enumerate(offsets):
        at = (first - 1 + n) * stride

        def mine(j, n=n, k=k, at=at):
            code = tables[0, 0, j]
            leaf = tables[first + n, 2, slot(code, k)]
            return lax.shift_right_logical(code, bits), at + 4 * leaf, leaf >= 0

        total = append(tables[0, 1, k], tables[0, 1, k + 1], mine, targets, sources, total)
        back = 7 - k

        def theirs(j, n=n, back=back, at=at):
            code = tables[first + n, 0, j]
            leaf = tables[0, 2, slot(code, back)]
            return leaf, at + 4 * lax.shift_right_logical(code, bits), leaf >= 0

        total = append(tables[first + n, 1, back], tables[first + n, 1, back + 1], theirs, targets, sources, total)
    return total


def self_kernel(own, acc, stacks, squares, weights, *, leaves):
    acc[...] = jnp.zeros_like(acc)
    size = 2 * squares.shape[0]

    def target_of(leaf):
        stack = target_stack(own[pl.ds(4 * leaf, 8), :])
        stacks[leaf] = stack
        return stack

    run_pairs(
        leaves // size,
        lambda i, u: i * size + u,
        lambda i, u: 4 * (i * size + u),
        target_of,
        own, acc, squares, weights,
    )


def load_parts(own, refs, pool, staging, tables, sem):
    stride = own.shape[0]
    parts = [(ref, row) for ref in refs for row in range(0, ref.shape[0], stride)]
    for n, (ref, row) in enumerate([(own, 0), *parts]):
        staging[n] = ref[pl.ds(row + stride - TABLE, TABLE), :].astype(jnp.int32)
    copy = pltpu.make_async_copy(staging, tables, sem)
    copy.start()
    for n, (ref, row) in enumerate(parts):
        pool[pl.ds(n * stride, stride), :] = ref[pl.ds(row, stride), :]
    return copy


def near_kernel(own, space_lower, space_upper, sub_a, sub_b, corner_a, stacks, acc_in, acc, pool, staging, tables, targets, sources, squares, weights, sem, *, leaves, sent, odd_of):
    rows = 4 * leaves
    stride = rows + TABLE
    odd = odd_of()
    copy = load_parts(own, (own, space_lower, space_upper, sub_a, sub_b, corner_a), pool, staging, tables, sem)
    acc[...] = acc_in[...]
    copy.wait()

    def both(j, n):
        code = tables[0, 0, j]
        t = lax.shift_right_logical(code, CODE.bit_length() - 1)
        u = code & (CODE - 1)
        targets[n] = t
        sources[n] = 4 * u
        targets[n + 1] = u
        sources[n + 1] = 4 * t
        return n + 2

    total = lax.fori_loop(tables[0, 1, LOCAL], tables[0, 1, LOCAL + 1], both, 0)
    offsets = (1, 6, 4 - odd, 3 + odd, 2 - 2 * odd, 7 - 2 * odd)
    total = append_ghosts(tables, offsets, 2, stride, targets, sources, total, leaves, sent)
    run_list(targets, sources, total, rows, stacks, pool, acc, squares, weights)


def far_kernel(own, corner_b, stacks, acc_in, out, acc, pool, staging, tables, targets, sources, squares, weights, sem, *, leaves, sent, odd_of):
    rows = 4 * leaves
    stride = rows + TABLE
    odd = odd_of()
    copy = load_parts(own, (corner_b,), pool, staging, tables, sem)
    acc[...] = acc_in[...]
    copy.wait()
    offsets = (2 * odd, 5 + 2 * odd)
    total = append_ghosts(tables, offsets, 1, stride, targets, sources, 0, leaves, sent)
    run_list(targets, sources, total, rows, stacks, pool, acc, squares, weights)

    def part(c):
        return acc[pl.ds(c, leaves, stride=8), :] + acc[pl.ds(c + 4, leaves, stride=8), :]

    mass = own[pl.ds(3, leaves, stride=4), :]
    norm = part(3)
    for c in range(3):
        out[c, 0] = mass * (part(c) - own[pl.ds(c, leaves, stride=4), :] * norm)


def ring(size, step):
    return [(i, (i + step) % size) for i in range(size)]


def both_ways(value, axis):
    size = lax.axis_size(axis)
    lower = lax.ppermute(value, axis, ring(size, 1))
    upper = lax.ppermute(value, axis, ring(size, -1))
    return lower, upper


def swaps(size, first):
    pairs = [(i, (i + 1) % size) for i in range(first, size, 2)]
    return pairs + [(j, i) for i, j in pairs]


def by_swaps(value, axis):
    size = lax.axis_size(axis)
    even = size % 2 == 0
    a = lax.ppermute(value, axis, swaps(size, 0) if even else ring(size, 1))
    b = lax.ppermute(value, axis, swaps(size, 1) if even else ring(size, -1))
    return a, b


def odd_index(axis):
    return lax.axis_index(axis) % 2 if lax.axis_size(axis) % 2 == 0 else jnp.int32(1)


def local(positions, masses, occupancy, export_slots, export_count, pair_list, pair_count):
    leaves, lanes = masses.shape[1:]
    sent = export_slots.shape[1]
    slots_of_pairs = pair_list.shape[2]
    rows = 4 * leaves + TABLE
    f32 = jnp.float32
    lane = lax.broadcasted_iota(jnp.int32, (1, lanes), 1)
    counts = jnp.where(lane < lanes // 2, export_count[0, 0], pair_count[0, 0])
    packed = pl.pallas_call(
        functools.partial(pack_kernel, leaves=leaves, sent=sent, slots_of_pairs=slots_of_pairs),
        out_shape=pltpu.VMEM((rows, lanes), f32),
        in_specs=[vmem()] * 6,
        out_specs=vmem(),
        name="pack",
    )(positions, masses, occupancy, export_slots, pair_list, on_chip(counts))

    def pairing(batch):
        return [
            pltpu.VMEM((batch // 2, lanes, 2 * lanes), f32),
            pltpu.VMEM((batch // 2, 32, lanes), jnp.bfloat16),
        ]

    def lists(parts, entries, batch):
        return [
            pltpu.VMEM((parts, TABLE, lanes), jnp.int32),
            pltpu.SMEM((parts, TABLE, lanes), jnp.int32),
            pltpu.SMEM((entries + batch + CHUNK,), jnp.int32),
            pltpu.SMEM((entries + batch + CHUNK,), jnp.int32),
            *pairing(batch),
            pltpu.SemaphoreType.DMA,
        ]

    def cost(blocks):
        return pl.CostEstimate(flops=blocks * lanes * lanes * 200, transcendentals=0, bytes_accessed=rows * lanes * 4)

    accumulator = pltpu.VMEM((8 * leaves, lanes), f32)
    sizes = dict(leaves=leaves, sent=sent, odd_of=functools.partial(odd_index, "sub"))
    space_lower, space_upper = both_ways(packed, "space")
    sub_a, sub_b = by_swaps(packed, "sub")
    acc, stacks = pl.pallas_call(
        functools.partial(self_kernel, leaves=leaves),
        out_shape=(accumulator, pltpu.VMEM((leaves, STACK, lanes), jnp.bfloat16)),
        in_specs=[vmem()],
        out_specs=(vmem(), vmem()),
        scratch_shapes=pairing(SELF_BATCH),
        cost_estimate=cost(leaves),
        name="self_pairs",
    )(on_chip(packed))
    corners = jnp.concatenate([space_lower, space_upper], axis=0)
    corner_a, corner_b = by_swaps(corners, "sub")
    acc = pl.pallas_call(
        functools.partial(near_kernel, **sizes),
        out_shape=accumulator,
        in_specs=[vmem()] * 8,
        out_specs=vmem(),
        scratch_shapes=[pltpu.VMEM((7 * rows, lanes), f32)]
        + lists(8, 8 * slots_of_pairs, NEAR_BATCH),
        cost_estimate=cost(slots_of_pairs),
        name="near_pairs",
    )(*map(on_chip, (packed, space_lower, space_upper, sub_a, sub_b, corner_a, stacks, acc)))
    return pl.pallas_call(
        functools.partial(far_kernel, **sizes),
        out_shape=jax.ShapeDtypeStruct((3, 1, leaves, lanes), f32),
        in_specs=[vmem()] * 4,
        out_specs=vmem(),
        scratch_shapes=[pltpu.VMEM((8 * leaves, lanes), f32), pltpu.VMEM((2 * rows, lanes), f32)]
        + lists(3, 3 * slots_of_pairs, FAR_BATCH),
        cost_estimate=cost(slots_of_pairs),
        name="far_pairs",
    )(*map(on_chip, (packed, corner_b, stacks, acc)))


def solution(mesh):
    return jax.shard_map(
        local,
        mesh=mesh,
        in_specs=(
            P(None, "space", "sub", None),
            P("space", "sub", None),
            P("space", "sub"),
            P("space", "sub"),
            P("space", "sub"),
            P(None, "space", "sub"),
            P("space", "sub"),
        ),
        out_specs=P(None, "space", "sub", None),
        check_vma=False,
    )
```

```python
import functools

import jax
import jax.numpy as jnp
from jax import lax
from jax.experimental import pallas as pl
from jax.experimental.pallas import tpu as pltpu
from jax.sharding import PartitionSpec as P


LOCAL = 8
SOFTEN = 0.05
CENTER = 0.75
TABLE = 8
CODE = 1024
SELF_BATCH, NEAR_BATCH, SENT_BATCH = 16, 12, 8
CHUNK = 4


def vmem():
    return pl.BlockSpec(memory_space=pltpu.VMEM)


def on_chip(value):
    return pltpu.with_memory_space_constraint(value, pltpu.VMEM)


def column(row, size):
    a = lax.broadcasted_iota(jnp.int32, (size, size), 0)
    b = lax.broadcasted_iota(jnp.int32, (size, size), 1)
    return jnp.sum(jnp.where(a == b, row[:, :size], 0), axis=1, keepdims=True)


def pack_kernel(pos, mass, occupancy, slots, pairs, counts, out, *, leaves, sent, slots_of_pairs):
    lanes = mass.shape[-1]
    occ = column(occupancy[...], leaves)
    lane = lax.broadcasted_iota(jnp.int32, (leaves, lanes), 1)
    live = jnp.where(lane < occ, mass[0], 0.0)
    for c in range(3):
        out[pl.ds(c, leaves, stride=4), :] = pos[c, 0] - CENTER
    out[pl.ds(3, leaves, stride=4), :] = live
    n = slots_of_pairs
    target = pairs[0]
    source = pairs[1]
    index = lax.broadcasted_iota(jnp.int32, (1, n), 1)
    key = jnp.where(source < leaves, LOCAL, (source - leaves) // sent)
    key = jnp.where(index < counts[:, lanes // 2 : lanes // 2 + 1], key, LOCAL + 1)
    code = target * CODE + source
    order = key * CODE + index
    order_col = column(order, n)
    code_col = column(code, n)
    rank = jnp.sum((order < order_col).astype(jnp.int32), axis=1, keepdims=True)
    place = lax.broadcasted_iota(jnp.int32, (n, lanes), 1)
    sorted_code = jnp.sum(jnp.where(place == rank, code_col, 0), axis=0, keepdims=True)
    starts = jnp.sum((order_col < place * CODE).astype(jnp.int32), axis=0, keepdims=True)
    g = lax.broadcasted_iota(jnp.int32, (1, sent), 1)
    alive = jnp.where(g < counts[:, 0:1], slots[...], -1)
    base = 4 * leaves
    out[pl.ds(base, TABLE), :] = jnp.zeros((TABLE, lanes), jnp.float32)
    out[pl.ds(base, 1), :] = sorted_code.astype(jnp.float32)
    out[pl.ds(base + 1, 1), :] = starts.astype(jnp.float32)
    out[pl.ds(base + 2, 1), :sent] = alive.astype(jnp.float32)


def split3(a):
    a1 = a.astype(jnp.bfloat16).astype(jnp.float32)
    r = a - a1
    a2 = r.astype(jnp.bfloat16).astype(jnp.float32)
    return a1, a2, r - a2


STACK = 48


def target_stack(target):
    row = lax.broadcasted_iota(jnp.int32, target.shape, 0)
    xt = jnp.where(row < 3, target, 0.0)
    qt = jnp.sum(xt * xt, axis=0, keepdims=True)
    b = jnp.where(row < 3, xt, jnp.where(row == 3, 1.0, jnp.where(row == 4, qt, 0.0)))
    b1, b2, b3 = split3(b)
    return jnp.concatenate([b1, b2, b1, b2, b3, b1], axis=0).astype(jnp.bfloat16)


def source_stacks(source):
    row = lax.broadcasted_iota(jnp.int32, source.shape, 0)
    xs = jnp.where(row < 3, source, 0.0)
    ms = source[3:4]
    qs = jnp.sum(xs * xs, axis=0, keepdims=True) + SOFTEN
    a = jnp.where(row < 3, -2.0 * xs, jnp.where(row == 3, qs, jnp.where(row == 4, 1.0, 0.0)))
    g = jnp.where(row < 3, xs * ms, jnp.where(row == 3, ms, 0.0))
    a1, a2, a3 = split3(a)
    g1, g2, g3 = split3(g)
    left = jnp.concatenate([a1, a1, a2, a2, a1, a3], axis=0).astype(jnp.bfloat16)
    moments = jnp.concatenate([g1 + pltpu.roll(g2, 4, 0), g3], axis=0).astype(jnp.bfloat16)
    return left, moments


def moment_sums(softened, moments):
    lanes = softened.shape[1] // 2
    inverse = lax.rsqrt(softened)
    scaled = jnp.maximum((1.0 + SOFTEN) - softened, 0.0) * inverse
    weight = scaled * scaled * inverse
    high = weight.astype(jnp.bfloat16)
    low = (weight - high.astype(jnp.float32)).astype(jnp.bfloat16)
    total = jnp.dot(
        jnp.concatenate([moments, moments], axis=1),
        jnp.concatenate([high, low], axis=0),
        preferred_element_type=jnp.float32,
    )
    return (
        total[0:8, :lanes] + total[8:16, :lanes],
        total[16:24, lanes:] + total[24:32, lanes:],
    )


def run_pairs(batches, first, second, target_of, pool, acc, squares, weights):
    lanes = pool.shape[1]
    size = 2 * squares.shape[0]
    none = jnp.zeros((STACK, lanes), jnp.bfloat16)

    def begin(i):
        begun = []
        for u in range(0, size, 2):
            rights = [target_of(first(i, v)) for v in (u, u + 1)]
            lefts = [source_stacks(pool[pl.ds(second(i, v), 8), :]) for v in (u, u + 1)]
            left = jnp.concatenate([lefts[0][0], lefts[1][0]], axis=0)
            right = jnp.concatenate(
                [
                    jnp.concatenate([rights[0], none], axis=1),
                    jnp.concatenate([none, rights[1]], axis=1),
                ],
                axis=0,
            )
            square = lax.dot_general(left, right, (((0,), (0,)), ((), ())), preferred_element_type=jnp.float32)
            begun.append((square, jnp.concatenate([lefts[0][1], lefts[1][1]], axis=0)))
        return begun

    def keep(begun):
        for unit, (square, moments) in enumerate(begun):
            squares[unit] = square
            weights[unit] = moments

    def finish():
        return [force for unit in range(size // 2) for force in moment_sums(squares[unit], weights[unit])]

    def add(i, sums):
        for u in range(size):
            at = pl.ds(pl.multiple_of(first(i, u) * 8, 8), 8)
            acc[at, :] += sums[u]

    def step(i, carry):
        begun = begin(i)
        sums = finish()
        keep(begun)
        add(i - 1, sums)
        return carry

    keep(begin(0))
    lax.fori_loop(1, batches, step, 0)
    add(batches - 1, finish())


def run_list(targets, sources, total, null_row, target_of, pool, acc, squares, weights):
    size = 2 * squares.shape[0]
    for u in range(size):
        targets[total + u] = 0
        sources[total + u] = null_row
    batches = jnp.maximum(lax.div(total + (size - 1), size), 1)
    run_pairs(
        batches,
        lambda i, u: targets[i * size + u],
        lambda i, u: sources[i * size + u],
        target_of,
        pool, acc, squares, weights,
    )


def append(begin, end, entry, targets, sources, total):
    def step(i, total):
        j = begin + i * CHUNK
        found = [entry(j + v) for v in range(CHUNK)]
        for v, (target, source, valid) in enumerate(found):
            targets[total] = target
            sources[total] = source
            total = total + jnp.where((j + v < end) & valid, 1, 0)
        return total

    return lax.fori_loop(0, lax.shift_right_logical(end - begin + (CHUNK - 1), CHUNK.bit_length() - 1), step, total)


def append_ghosts(tables, offsets, first, row, stride, targets, sources, total, leaves, sent):
    lanes = tables.shape[2]
    bits = CODE.bit_length() - 1

    def slot(code, k):
        return ((code & (CODE - 1)) - (leaves + k * sent)) & (lanes - 1)

    for n, k in enumerate(offsets):
        at = row + n * stride

        def mine(j, n=n, k=k, at=at):
            code = tables[0, 0, j]
            leaf = tables[first + n, 2, slot(code, k)]
            return lax.shift_right_logical(code, bits), at + 4 * leaf, leaf >= 0

        total = append(tables[0, 1, k], tables[0, 1, k + 1], mine, targets, sources, total)
        back = 7 - k

        def theirs(j, n=n, back=back, at=at):
            code = tables[first + n, 0, j]
            leaf = tables[0, 2, slot(code, back)]
            return leaf, at + 4 * lax.shift_right_logical(code, bits), leaf >= 0

        total = append(tables[first + n, 1, back], tables[first + n, 1, back + 1], theirs, targets, sources, total)
    return total


def self_kernel(own, acc, stacks, squares, weights, *, leaves):
    acc[...] = jnp.zeros_like(acc)
    size = 2 * squares.shape[0]

    def target_of(leaf):
        stack = target_stack(own[pl.ds(4 * leaf, 8), :])
        stacks[leaf] = stack
        return stack

    run_pairs(
        leaves // size,
        lambda i, u: i * size + u,
        lambda i, u: 4 * (i * size + u),
        target_of,
        own, acc, squares, weights,
    )


def fetch_tables(parts, staging, tables, sem):
    for n, (ref, row) in enumerate(parts):
        staging[n] = ref[pl.ds(row, TABLE), :].astype(jnp.int32)
    copy = pltpu.make_async_copy(staging, tables, sem)
    copy.start()
    return copy


def forces(acc, packed, leaves):
    def part(c):
        return acc[pl.ds(c, leaves, stride=8), :] + acc[pl.ds(c + 4, leaves, stride=8), :]

    mass = packed[pl.ds(3, leaves, stride=4), :]
    norm = part(3)
    return [mass * (part(c) - packed[pl.ds(c, leaves, stride=4), :] * norm) for c in range(3)]


def sent_kernel(sub_b, corners, out, acc, staging, tables, targets, sources, squares, weights, sem, *, leaves, sent, index_of):
    rows = 4 * leaves
    stride = rows + TABLE
    odd = lax.rem(index_of(), 2)
    copy = fetch_tables([(sub_b, rows), (corners, rows), (corners, stride + rows)], staging, tables, sem)
    acc[...] = jnp.zeros_like(acc)
    copy.wait()
    offsets = (2 - 2 * odd, 7 - 2 * odd)
    total = append_ghosts(tables, offsets, 1, 0, stride, targets, sources, 0, leaves, sent)
    run_list(
        targets, sources, total, rows,
        lambda leaf: target_stack(sub_b[pl.ds(4 * leaf, 8), :]),
        corners, acc, squares, weights,
    )
    for c, force in enumerate(forces(acc, sub_b, leaves)):
        out[c] = force


def near_kernel(own, space_lower, space_upper, sub_a, sub_b, corner_a, stacks, acc_in, out, acc, pool, staging, tables, targets, sources, squares, weights, sem, *, leaves, sent, index_of):
    rows = 4 * leaves
    stride = rows + TABLE
    odd = lax.rem(index_of(), 2)
    parts = [(own, 0), (space_lower, 0), (space_upper, 0), (sub_a, 0), (sub_b, 0), (corner_a, 0), (corner_a, stride)]
    copy = fetch_tables([(ref, row + rows) for ref, row in parts], staging, tables, sem)
    acc[...] = acc_in[...]
    for n, (ref, row) in enumerate(parts):
        pool[pl.ds(n * stride, stride), :] = ref[pl.ds(row, stride), :]
    copy.wait()

    def both(j, n):
        code = tables[0, 0, j]
        t = lax.shift_right_logical(code, CODE.bit_length() - 1)
        u = code & (CODE - 1)
        targets[n] = t
        sources[n] = 4 * u
        targets[n + 1] = u
        sources[n + 1] = 4 * t
        return n + 2

    total = lax.fori_loop(tables[0, 1, LOCAL], tables[0, 1, LOCAL + 1], both, 0)
    offsets = (1, 6, 4 - odd, 3 + odd, 2 - 2 * odd, 7 - 2 * odd)
    total = append_ghosts(tables, offsets, 1, stride, stride, targets, sources, total, leaves, sent)
    run_list(targets, sources, total, rows, lambda leaf: stacks[leaf], pool, acc, squares, weights)
    for c, force in enumerate(forces(acc, own, leaves)):
        out[c] = force


def ring(size, step):
    return [(i, (i + step) % size) for i in range(size)]


def both_ways(value, axis):
    size = lax.axis_size(axis)
    lower = lax.ppermute(value, axis, ring(size, 1))
    upper = lax.ppermute(value, axis, ring(size, -1))
    return lower, upper


def swapped(value, axis, first):
    size = lax.axis_size(axis)
    pairs = [(i, (i + 1) % size) for i in range(first, size, 2)]
    return lax.ppermute(value, axis, pairs + [(j, i) for i, j in pairs])


def local(positions, masses, occupancy, export_slots, export_count, pair_list, pair_count):
    leaves, lanes = masses.shape[1:]
    sent = export_slots.shape[1]
    slots_of_pairs = pair_list.shape[2]
    rows = 4 * leaves + TABLE
    f32 = jnp.float32
    lane = lax.broadcasted_iota(jnp.int32, (1, lanes), 1)
    counts = jnp.where(lane < lanes // 2, export_count[0, 0], pair_count[0, 0])
    packed = pl.pallas_call(
        functools.partial(pack_kernel, leaves=leaves, sent=sent, slots_of_pairs=slots_of_pairs),
        out_shape=pltpu.VMEM((rows, lanes), f32),
        in_specs=[vmem()] * 6,
        out_specs=vmem(),
        name="pack",
    )(positions, masses, occupancy, export_slots, pair_list, on_chip(counts))

    def pairing(batch):
        return [
            pltpu.VMEM((batch // 2, lanes, 2 * lanes), f32),
            pltpu.VMEM((batch // 2, 32, lanes), jnp.bfloat16),
        ]

    def lists(parts, entries, batch):
        return [
            pltpu.VMEM((parts, TABLE, lanes), jnp.int32),
            pltpu.SMEM((parts, TABLE, lanes), jnp.int32),
            pltpu.SMEM((entries + batch + CHUNK,), jnp.int32),
            pltpu.SMEM((entries + batch + CHUNK,), jnp.int32),
            *pairing(batch),
            pltpu.SemaphoreType.DMA,
        ]

    def cost(blocks):
        return pl.CostEstimate(flops=blocks * lanes * lanes * 200, transcendentals=0, bytes_accessed=rows * lanes * 4)

    accumulator = pltpu.VMEM((8 * leaves, lanes), f32)
    force = pltpu.VMEM((3, leaves, lanes), f32)
    sizes = dict(leaves=leaves, sent=sent, index_of=functools.partial(lax.axis_index, "sub"))
    space_lower, space_upper = both_ways(packed, "space")
    sub_a = swapped(packed, "sub", 0)
    sub_b = swapped(packed, "sub", 1)
    acc, stacks = pl.pallas_call(
        functools.partial(self_kernel, leaves=leaves),
        out_shape=(accumulator, pltpu.VMEM((leaves, STACK, lanes), jnp.bfloat16)),
        in_specs=[vmem()],
        out_specs=(vmem(), vmem()),
        scratch_shapes=pairing(SELF_BATCH),
        cost_estimate=cost(leaves),
        name="self_pairs",
    )(on_chip(packed))
    corners = jnp.concatenate([space_lower, space_upper], axis=0)
    corner_a = swapped(corners, "sub", 0)
    for_b = pl.pallas_call(
        functools.partial(sent_kernel, **sizes),
        out_shape=force,
        in_specs=[vmem()] * 2,
        out_specs=vmem(),
        scratch_shapes=[pltpu.VMEM((8 * leaves, lanes), f32)] + lists(3, 3 * slots_of_pairs, SENT_BATCH),
        cost_estimate=cost(slots_of_pairs),
        name="sent_pairs",
    )(*map(on_chip, (sub_b, corners)))
    from_b = swapped(for_b, "sub", 1)
    near = pl.pallas_call(
        functools.partial(near_kernel, **sizes),
        out_shape=force,
        in_specs=[vmem()] * 8,
        out_specs=vmem(),
        scratch_shapes=[pltpu.VMEM((8 * leaves, lanes), f32), pltpu.VMEM((7 * rows, lanes), f32)]
        + lists(7, 8 * slots_of_pairs, NEAR_BATCH),
        cost_estimate=cost(slots_of_pairs),
        name="near_pairs",
    )(*map(on_chip, (packed, space_lower, space_upper, sub_a, sub_b, corner_a, stacks, acc)))
    return (near + from_b)[:, None]


def solution(mesh):
    return jax.shard_map(
        local,
        mesh=mesh,
        in_specs=(
            P(None, "space", "sub", None),
            P("space", "sub", None),
            P("space", "sub"),
            P("space", "sub"),
            P("space", "sub"),
            P(None, "space", "sub"),
            P("space", "sub"),
        ),
        out_specs=P(None, "space", "sub", None),
        check_vma=False,
    )
```

```python
import functools

import jax
import jax.numpy as jnp
from jax import lax
from jax.experimental import pallas as pl
from jax.experimental.pallas import tpu as pltpu
from jax.sharding import PartitionSpec as P


LOCAL = 8
SOFTEN = 0.05
CENTER = 0.75
TABLE = 8
CODE = 1024
SELF_BATCH, NEAR_BATCH, SENT_BATCH = 16, 8, 8
CHUNK = 4


def vmem():
    return pl.BlockSpec(memory_space=pltpu.VMEM)


def on_chip(value):
    return pltpu.with_memory_space_constraint(value, pltpu.VMEM)


def column(row, size):
    a = lax.broadcasted_iota(jnp.int32, (size, size), 0)
    b = lax.broadcasted_iota(jnp.int32, (size, size), 1)
    return jnp.sum(jnp.where(a == b, row[:, :size], 0), axis=1, keepdims=True)


def pack_kernel(pos, mass, occupancy, slots, pairs, counts, out, *, leaves, sent, slots_of_pairs):
    lanes = mass.shape[-1]
    occ = column(occupancy[...], leaves)
    lane = lax.broadcasted_iota(jnp.int32, (leaves, lanes), 1)
    live = jnp.where(lane < occ, mass[0], 0.0)
    for c in range(3):
        out[pl.ds(c, leaves, stride=4), :] = pos[c, 0] - CENTER
    out[pl.ds(3, leaves, stride=4), :] = live
    n = slots_of_pairs
    target = pairs[0]
    source = pairs[1]
    index = lax.broadcasted_iota(jnp.int32, (1, n), 1)
    key = jnp.where(source < leaves, LOCAL, (source - leaves) // sent)
    key = jnp.where(index < counts[:, lanes // 2 : lanes // 2 + 1], key, LOCAL + 1)
    code = target * CODE + source
    order = key * CODE + index
    order_col = column(order, n)
    code_col = column(code, n)
    rank = jnp.sum((order < order_col).astype(jnp.int32), axis=1, keepdims=True)
    place = lax.broadcasted_iota(jnp.int32, (n, lanes), 1)
    sorted_code = jnp.sum(jnp.where(place == rank, code_col, 0), axis=0, keepdims=True)
    at_slots, at_starts = table_places(n, sent)
    key_place = place - at_starts
    starts = jnp.sum(((order_col < key_place * CODE) & (key_place > 0)).astype(jnp.int32), axis=0, keepdims=True)
    g = lax.broadcasted_iota(jnp.int32, (1, sent), 1)
    alive = column(jnp.where(g < counts[:, 0:1], slots[...], -1), sent)
    slot_place = lax.broadcasted_iota(jnp.int32, (sent, lanes), 1) - at_slots
    slot = lax.broadcasted_iota(jnp.int32, (sent, lanes), 0)
    table = sorted_code + starts + jnp.sum(jnp.where(slot_place == slot, alive, 0), axis=0, keepdims=True)
    base = 4 * leaves
    out[pl.ds(base, TABLE), :] = jnp.zeros((TABLE, lanes), jnp.float32)
    out[pl.ds(base, 1), :] = table.astype(jnp.float32)


def table_places(pairs, sent):
    at_slots = pairs
    return at_slots, at_slots + (1 << (sent - 1).bit_length())


def split3(a):
    a1 = a.astype(jnp.bfloat16).astype(jnp.float32)
    r = a - a1
    a2 = r.astype(jnp.bfloat16).astype(jnp.float32)
    return a1, a2, r - a2


STACK = 48


def target_stack(target):
    row = lax.broadcasted_iota(jnp.int32, target.shape, 0)
    xt = jnp.where(row < 3, target, 0.0)
    qt = jnp.sum(xt * xt, axis=0, keepdims=True)
    b = jnp.where(row < 3, xt, jnp.where(row == 3, 1.0, jnp.where(row == 4, qt, 0.0)))
    b1, b2, b3 = split3(b)
    return jnp.concatenate([b1, b2, b1, b2, b3, b1], axis=0).astype(jnp.bfloat16)


def source_stacks(source):
    row = lax.broadcasted_iota(jnp.int32, source.shape, 0)
    xs = jnp.where(row < 3, source, 0.0)
    ms = source[3:4]
    qs = jnp.sum(xs * xs, axis=0, keepdims=True) + SOFTEN
    a = jnp.where(row < 3, -2.0 * xs, jnp.where(row == 3, qs, jnp.where(row == 4, 1.0, 0.0)))
    g = jnp.where(row < 3, xs * ms, jnp.where(row == 3, ms, 0.0))
    a1, a2, a3 = split3(a)
    g1, g2, g3 = split3(g)
    left = jnp.concatenate([a1, a1, a2, a2, a1, a3], axis=0).astype(jnp.bfloat16)
    moments = jnp.concatenate([g1 + pltpu.roll(g2, 4, 0), g3], axis=0).astype(jnp.bfloat16)
    return left, moments


def factors(softened):
    inverse = lax.rsqrt(softened)
    scaled = jnp.maximum((1.0 + SOFTEN) - softened, 0.0) * inverse
    weight = scaled * scaled * inverse
    high = weight.astype(jnp.bfloat16)
    low = (weight - high.astype(jnp.float32)).astype(jnp.bfloat16)
    return jnp.concatenate([high, low], axis=0)


def moment_sums(factor, moments):
    lanes = factor.shape[1] // 2
    total = jnp.dot(
        jnp.concatenate([moments, moments], axis=1), factor, preferred_element_type=jnp.float32
    )
    return (
        total[0:8, :lanes] + total[8:16, :lanes],
        total[16:24, lanes:] + total[24:32, lanes:],
    )


def run_pairs(batches, first, second, target_of, pool, acc, squares, weights, *later):
    lanes = pool.shape[1]
    units = range(squares.shape[0])
    size = 2 * len(units)
    none = jnp.zeros((STACK, lanes), jnp.bfloat16)

    def begin(i):
        begun = []
        for u in range(0, size, 2):
            rights = [target_of(first(i, v)) for v in (u, u + 1)]
            lefts = [source_stacks(pool[pl.ds(second(i, v), 8), :]) for v in (u, u + 1)]
            left = jnp.concatenate([lefts[0][0], lefts[1][0]], axis=0)
            right = jnp.concatenate(
                [
                    jnp.concatenate([rights[0], none], axis=1),
                    jnp.concatenate([none, rights[1]], axis=1),
                ],
                axis=0,
            )
            square = lax.dot_general(left, right, (((0,), (0,)), ((), ())), preferred_element_type=jnp.float32)
            begun.append((square, jnp.concatenate([lefts[0][1], lefts[1][1]], axis=0)))
        return begun

    def keep(begun):
        for unit, (square, moments) in enumerate(begun):
            squares[unit] = square
            weights[unit] = moments

    def middle():
        return [(factors(squares[unit]), weights[unit]) for unit in units]

    def keep_middle(made):
        for unit, (factor, moments) in enumerate(made):
            later[0][unit] = factor
            later[1][unit] = moments

    def finish(made):
        return [force for factor, moments in made for force in moment_sums(factor, moments)]

    def last():
        return finish([(later[0][unit], later[1][unit]) for unit in units])

    def add(i, sums):
        for u in range(size):
            at = pl.ds(pl.multiple_of(first(i, u) * 8, 8), 8)
            acc[at, :] += sums[u]

    def step(i, carry):
        begun = begin(i)
        sums = finish(middle())
        keep(begun)
        add(i - 1, sums)
        return carry

    def deep_step(i, carry):
        begun = begin(i)
        sums = last()
        made = middle()
        keep_middle(made)
        keep(begun)
        add(i - 2, sums)
        return carry

    keep(begin(0))
    if not later:
        lax.fori_loop(1, batches, step, 0)
        add(batches - 1, finish(middle()))
        return
    begun = begin(1)
    made = middle()
    keep_middle(made)
    keep(begun)
    lax.fori_loop(2, batches, deep_step, 0)
    sums = last()
    made = middle()
    keep_middle(made)
    add(batches - 2, sums)
    add(batches - 1, last())


def run_list(targets, sources, total, null_row, target_of, pool, acc, squares, weights, *later):
    size = 2 * squares.shape[0]
    least = 2 if later else 1
    for u in range(least * size):
        targets[total + u] = 0
        sources[total + u] = null_row
    batches = jnp.maximum(lax.div(total + (size - 1), size), least)
    run_pairs(
        batches,
        lambda i, u: targets[i * size + u],
        lambda i, u: sources[i * size + u],
        target_of,
        pool, acc, squares, weights, *later,
    )


def append(begin, end, entry, targets, sources, total):
    def step(i, total):
        j = begin + i * CHUNK
        found = [entry(j + v) for v in range(CHUNK)]
        for v, (target, source, valid) in enumerate(found):
            targets[total] = target
            sources[total] = source
            total = total + jnp.where((j + v < end) & valid, 1, 0)
        return total

    return lax.fori_loop(0, lax.shift_right_logical(end - begin + (CHUNK - 1), CHUNK.bit_length() - 1), step, total)


def append_ghosts(tables, offsets, first, row, stride, targets, sources, total, leaves, sent, pairs):
    at_slots, at_starts = table_places(pairs, sent)
    bits = CODE.bit_length() - 1

    def slot(code, k):
        return at_slots + (((code & (CODE - 1)) - (leaves + k * sent)) & (at_starts - at_slots - 1))

    for n, k in enumerate(offsets):
        at = row + n * stride

        def mine(j, n=n, k=k, at=at):
            code = tables[0, j]
            leaf = tables[first + n, slot(code, k)]
            return lax.shift_right_logical(code, bits), at + 4 * leaf, leaf >= 0

        total = append(tables[0, at_starts + k], tables[0, at_starts + k + 1], mine, targets, sources, total)
        back = 7 - k

        def theirs(j, n=n, back=back, at=at):
            code = tables[first + n, j]
            leaf = tables[0, slot(code, back)]
            return leaf, at + 4 * lax.shift_right_logical(code, bits), leaf >= 0

        total = append(tables[first + n, at_starts + back], tables[first + n, at_starts + back + 1], theirs, targets, sources, total)
    return total


def self_kernel(own, acc, stacks, squares, weights, factor, moments, *, leaves):
    acc[...] = jnp.zeros_like(acc)
    size = 2 * squares.shape[0]

    def target_of(leaf):
        stack = target_stack(own[pl.ds(4 * leaf, 8), :])
        stacks[leaf] = stack
        return stack

    run_pairs(
        leaves // size,
        lambda i, u: i * size + u,
        lambda i, u: 4 * (i * size + u),
        target_of,
        own, acc, squares, weights, factor, moments,
    )


def fetch_tables(parts, staging, tables, sem):
    for n, (ref, row) in enumerate(parts):
        staging[pl.ds(n, 1), :] = ref[pl.ds(row, 1), :].astype(jnp.int32)
    copy = pltpu.make_async_copy(staging, tables, sem)
    copy.start()
    return copy


def forces(acc, packed, leaves):
    def part(c):
        return acc[pl.ds(c, leaves, stride=8), :] + acc[pl.ds(c + 4, leaves, stride=8), :]

    mass = packed[pl.ds(3, leaves, stride=4), :]
    norm = part(3)
    return [mass * (part(c) - packed[pl.ds(c, leaves, stride=4), :] * norm) for c in range(3)]


def sent_kernel(sub_b, corners, out, acc, staging, tables, targets, sources, squares, weights, sem, *, leaves, sent, pairs, index_of):
    rows = 4 * leaves
    stride = rows + TABLE
    odd = lax.rem(index_of(), 2)
    copy = fetch_tables([(sub_b, rows), (corners, rows), (corners, stride + rows)], staging, tables, sem)
    acc[...] = jnp.zeros_like(acc)
    copy.wait()
    offsets = (2 - 2 * odd, 7 - 2 * odd)
    total = append_ghosts(tables, offsets, 1, 0, stride, targets, sources, 0, leaves, sent, pairs)
    run_list(
        targets, sources, total, rows,
        lambda leaf: target_stack(sub_b[pl.ds(4 * leaf, 8), :]),
        corners, acc, squares, weights,
    )
    for c, force in enumerate(forces(acc, sub_b, leaves)):
        out[c] = force


def near_kernel(own, space_lower, space_upper, sub_a, sub_b, corner_a, stacks, acc_in, out, acc, pool, staging, tables, targets, sources, squares, weights, factor, moments, sem, *, leaves, sent, pairs, index_of):
    rows = 4 * leaves
    stride = rows + TABLE
    odd = lax.rem(index_of(), 2)
    parts = [(own, 0), (space_lower, 0), (space_upper, 0), (sub_a, 0), (sub_b, 0), (corner_a, 0), (corner_a, stride)]
    copy = fetch_tables([(ref, row + rows) for ref, row in parts], staging, tables, sem)
    acc[...] = acc_in[...]
    for n, (ref, row) in enumerate(parts):
        pool[pl.ds(n * stride, stride), :] = ref[pl.ds(row, stride), :]
    copy.wait()

    at_starts = table_places(pairs, sent)[1]

    def both(j, n):
        code = tables[0, j]
        t = lax.shift_right_logical(code, CODE.bit_length() - 1)
        u = code & (CODE - 1)
        targets[n] = t
        sources[n] = 4 * u
        targets[n + 1] = u
        sources[n + 1] = 4 * t
        return n + 2

    total = lax.fori_loop(tables[0, at_starts + LOCAL], tables[0, at_starts + LOCAL + 1], both, 0)
    offsets = (1, 6, 4 - odd, 3 + odd, 2 - 2 * odd, 7 - 2 * odd)
    total = append_ghosts(tables, offsets, 1, stride, stride, targets, sources, total, leaves, sent, pairs)
    run_list(targets, sources, total, rows, lambda leaf: stacks[leaf], pool, acc, squares, weights, factor, moments)
    for c, force in enumerate(forces(acc, own, leaves)):
        out[c] = force


def ring(size, step):
    return [(i, (i + step) % size) for i in range(size)]


def both_ways(value, axis):
    size = lax.axis_size(axis)
    lower = lax.ppermute(value, axis, ring(size, 1))
    upper = lax.ppermute(value, axis, ring(size, -1))
    return lower, upper


def swapped(value, axis, first):
    size = lax.axis_size(axis)
    pairs = [(i, (i + 1) % size) for i in range(first, size, 2)]
    return lax.ppermute(value, axis, pairs + [(j, i) for i, j in pairs])


def local(positions, masses, occupancy, export_slots, export_count, pair_list, pair_count):
    leaves, lanes = masses.shape[1:]
    sent = export_slots.shape[1]
    slots_of_pairs = pair_list.shape[2]
    rows = 4 * leaves + TABLE
    f32 = jnp.float32
    lane = lax.broadcasted_iota(jnp.int32, (1, lanes), 1)
    counts = jnp.where(lane < lanes // 2, export_count[0, 0], pair_count[0, 0])
    packed = pl.pallas_call(
        functools.partial(pack_kernel, leaves=leaves, sent=sent, slots_of_pairs=slots_of_pairs),
        out_shape=pltpu.VMEM((rows, lanes), f32),
        in_specs=[vmem()] * 6,
        out_specs=vmem(),
        name="pack",
    )(positions, masses, occupancy, export_slots, pair_list, on_chip(counts))

    def pairing(batch, deep):
        stages = [
            pltpu.VMEM((batch // 2, lanes, 2 * lanes), f32),
            pltpu.VMEM((batch // 2, 32, lanes), jnp.bfloat16),
        ]
        if deep:
            stages += [
                pltpu.VMEM((batch // 2, 2 * lanes, 2 * lanes), jnp.bfloat16),
                pltpu.VMEM((batch // 2, 32, lanes), jnp.bfloat16),
            ]
        return stages

    def lists(parts, entries, batch, deep):
        return [
            pltpu.VMEM((parts, lanes), jnp.int32),
            pltpu.SMEM((parts, lanes), jnp.int32),
            pltpu.SMEM((entries + 2 * batch + CHUNK,), jnp.int32),
            pltpu.SMEM((entries + 2 * batch + CHUNK,), jnp.int32),
            *pairing(batch, deep),
            pltpu.SemaphoreType.DMA,
        ]

    def cost(blocks):
        return pl.CostEstimate(flops=blocks * lanes * lanes * 200, transcendentals=0, bytes_accessed=rows * lanes * 4)

    accumulator = pltpu.VMEM((8 * leaves, lanes), f32)
    force = pltpu.VMEM((3, leaves, lanes), f32)
    sizes = dict(leaves=leaves, sent=sent, pairs=slots_of_pairs, index_of=functools.partial(lax.axis_index, "sub"))
    space_lower, space_upper = both_ways(packed, "space")
    sub_a = swapped(packed, "sub", 0)
    sub_b = swapped(packed, "sub", 1)
    acc, stacks = pl.pallas_call(
        functools.partial(self_kernel, leaves=leaves),
        out_shape=(accumulator, pltpu.VMEM((leaves, STACK, lanes), jnp.bfloat16)),
        in_specs=[vmem()],
        out_specs=(vmem(), vmem()),
        scratch_shapes=pairing(SELF_BATCH, True),
        cost_estimate=cost(leaves),
        name="self_pairs",
    )(on_chip(packed))
    corners = jnp.concatenate([space_lower, space_upper], axis=0)
    corner_a = swapped(corners, "sub", 0)
    for_b = pl.pallas_call(
        functools.partial(sent_kernel, **sizes),
        out_shape=force,
        in_specs=[vmem()] * 2,
        out_specs=vmem(),
        scratch_shapes=[pltpu.VMEM((8 * leaves, lanes), f32)] + lists(3, 3 * slots_of_pairs, SENT_BATCH, False),
        cost_estimate=cost(slots_of_pairs),
        name="sent_pairs",
    )(*map(on_chip, (sub_b, corners)))
    from_b = swapped(for_b, "sub", 1)
    near = pl.pallas_call(
        functools.partial(near_kernel, **sizes),
        out_shape=force,
        in_specs=[vmem()] * 8,
        out_specs=vmem(),
        scratch_shapes=[pltpu.VMEM((8 * leaves, lanes), f32), pltpu.VMEM((7 * rows, lanes), f32)]
        + lists(7, 8 * slots_of_pairs, NEAR_BATCH, True),
        cost_estimate=cost(slots_of_pairs),
        name="near_pairs",
    )(*map(on_chip, (packed, space_lower, space_upper, sub_a, sub_b, corner_a, stacks, acc)))
    return (near + from_b)[:, None]


def solution(mesh):
    return jax.shard_map(
        local,
        mesh=mesh,
        in_specs=(
            P(None, "space", "sub", None),
            P("space", "sub", None),
            P("space", "sub"),
            P("space", "sub"),
            P("space", "sub"),
            P(None, "space", "sub"),
            P("space", "sub"),
        ),
        out_specs=P(None, "space", "sub", None),
        check_vma=False,
    )
```

```python
import functools

import jax
import jax.numpy as jnp
from jax import lax
from jax.experimental import pallas as pl
from jax.experimental.pallas import tpu as pltpu
from jax.sharding import PartitionSpec as P


LOCAL = 8
SOFTEN = 0.05
CENTER = 0.75
TABLE = 8
CODE = 1024
OWN_BATCH, NEAR_BATCH, SENT_BATCH = 16, 8, 8
CHUNK = 4


def vmem():
    return pl.BlockSpec(memory_space=pltpu.VMEM)


def on_chip(value):
    return pltpu.with_memory_space_constraint(value, pltpu.VMEM)


def column(row, size):
    a = lax.broadcasted_iota(jnp.int32, (size, size), 0)
    b = lax.broadcasted_iota(jnp.int32, (size, size), 1)
    return jnp.sum(jnp.where(a == b, row[:, :size], 0), axis=1, keepdims=True)


def pack_kernel(pos, mass, occupancy, slots, pairs, counts, out, *, leaves, sent, slots_of_pairs):
    lanes = mass.shape[-1]
    occ = column(occupancy[...], leaves)
    lane = lax.broadcasted_iota(jnp.int32, (leaves, lanes), 1)
    live = jnp.where(lane < occ, mass[0], 0.0)
    for c in range(3):
        out[pl.ds(c, leaves, stride=4), :] = pos[c, 0] - CENTER
    out[pl.ds(3, leaves, stride=4), :] = live
    n = slots_of_pairs
    target = pairs[0]
    source = pairs[1]
    index = lax.broadcasted_iota(jnp.int32, (1, n), 1)
    key = jnp.where(source < leaves, LOCAL, (source - leaves) // sent)
    key = jnp.where(index < counts[:, lanes // 2 : lanes // 2 + 1], key, LOCAL + 1)
    code = target * CODE + source
    order = key * CODE + index
    order_col = column(order, n)
    code_col = column(code, n)
    rank = jnp.sum((order < order_col).astype(jnp.int32), axis=1, keepdims=True)
    place = lax.broadcasted_iota(jnp.int32, (n, lanes), 1)
    sorted_code = jnp.sum(jnp.where(place == rank, code_col, 0), axis=0, keepdims=True)
    at_slots, at_starts = table_places(n, sent)
    key_place = place - at_starts
    starts = jnp.sum(((order_col < key_place * CODE) & (key_place > 0)).astype(jnp.int32), axis=0, keepdims=True)
    g = lax.broadcasted_iota(jnp.int32, (1, sent), 1)
    alive = column(jnp.where(g < counts[:, 0:1], slots[...], -1), sent)
    slot_place = lax.broadcasted_iota(jnp.int32, (sent, lanes), 1) - at_slots
    slot = lax.broadcasted_iota(jnp.int32, (sent, lanes), 0)
    table = sorted_code + starts + jnp.sum(jnp.where(slot_place == slot, alive, 0), axis=0, keepdims=True)
    base = 4 * leaves
    out[pl.ds(base, TABLE), :] = jnp.zeros((TABLE, lanes), jnp.float32)
    out[pl.ds(base, 1), :] = table.astype(jnp.float32)


def table_places(pairs, sent):
    at_slots = pairs
    return at_slots, at_slots + (1 << (sent - 1).bit_length())


def split3(a):
    a1 = a.astype(jnp.bfloat16).astype(jnp.float32)
    r = a - a1
    a2 = r.astype(jnp.bfloat16).astype(jnp.float32)
    return a1, a2, r - a2


STACK = 48


def target_stack(target):
    row = lax.broadcasted_iota(jnp.int32, target.shape, 0)
    xt = jnp.where(row < 3, target, 0.0)
    qt = jnp.sum(xt * xt, axis=0, keepdims=True)
    b = jnp.where(row < 3, xt, jnp.where(row == 3, 1.0, jnp.where(row == 4, qt, 0.0)))
    b1, b2, b3 = split3(b)
    return jnp.concatenate([b1, b2, b1, b2, b3, b1], axis=0).astype(jnp.bfloat16)


def source_stacks(source):
    row = lax.broadcasted_iota(jnp.int32, source.shape, 0)
    xs = jnp.where(row < 3, source, 0.0)
    ms = source[3:4]
    qs = jnp.sum(xs * xs, axis=0, keepdims=True) + SOFTEN
    a = jnp.where(row < 3, -2.0 * xs, jnp.where(row == 3, qs, jnp.where(row == 4, 1.0, 0.0)))
    g = jnp.where(row < 3, xs * ms, jnp.where(row == 3, ms, 0.0))
    a1, a2, a3 = split3(a)
    g1, g2, g3 = split3(g)
    left = jnp.concatenate([a1, a1, a2, a2, a1, a3], axis=0).astype(jnp.bfloat16)
    moments = jnp.concatenate([g1 + pltpu.roll(g2, 4, 0), g3], axis=0).astype(jnp.bfloat16)
    return left, moments


def factors(softened):
    inverse = lax.rsqrt(softened)
    scaled = jnp.maximum((1.0 + SOFTEN) - softened, 0.0) * inverse
    weight = scaled * scaled * inverse
    high = weight.astype(jnp.bfloat16)
    low = (weight - high.astype(jnp.float32)).astype(jnp.bfloat16)
    return jnp.concatenate([high, low], axis=0)


def moment_sums(factor, moments):
    lanes = factor.shape[1] // 2
    total = jnp.dot(
        jnp.concatenate([moments, moments], axis=1), factor, preferred_element_type=jnp.float32
    )
    return (
        total[0:8, :lanes] + total[8:16, :lanes],
        total[16:24, lanes:] + total[24:32, lanes:],
    )


def run_pairs(batches, first, second, target_of, pool, acc, squares, weights, *later):
    lanes = pool.shape[1]
    units = range(squares.shape[0])
    size = 2 * len(units)
    none = jnp.zeros((STACK, lanes), jnp.bfloat16)

    def begin(i):
        begun = []
        for u in range(0, size, 2):
            rights = [target_of(first(i, v)) for v in (u, u + 1)]
            lefts = [source_stacks(pool[pl.ds(second(i, v), 8), :]) for v in (u, u + 1)]
            left = jnp.concatenate([lefts[0][0], lefts[1][0]], axis=0)
            right = jnp.concatenate(
                [
                    jnp.concatenate([rights[0], none], axis=1),
                    jnp.concatenate([none, rights[1]], axis=1),
                ],
                axis=0,
            )
            square = lax.dot_general(left, right, (((0,), (0,)), ((), ())), preferred_element_type=jnp.float32)
            begun.append((square, jnp.concatenate([lefts[0][1], lefts[1][1]], axis=0)))
        return begun

    def keep(begun):
        for unit, (square, moments) in enumerate(begun):
            squares[unit] = square
            weights[unit] = moments

    def middle():
        return [(factors(squares[unit]), weights[unit]) for unit in units]

    def keep_middle(made):
        for unit, (factor, moments) in enumerate(made):
            later[0][unit] = factor
            later[1][unit] = moments

    def finish(made):
        return [force for factor, moments in made for force in moment_sums(factor, moments)]

    def last():
        return finish([(later[0][unit], later[1][unit]) for unit in units])

    def add(i, sums):
        for u in range(size):
            at = pl.ds(pl.multiple_of(first(i, u) * 8, 8), 8)
            acc[at, :] += sums[u]

    def step(i, carry):
        begun = begin(i)
        sums = finish(middle())
        keep(begun)
        add(i - 1, sums)
        return carry

    def deep_step(i, carry):
        begun = begin(i)
        sums = last()
        made = middle()
        keep_middle(made)
        keep(begun)
        add(i - 2, sums)
        return carry

    keep(begin(0))
    if not later:
        lax.fori_loop(1, batches, step, 0)
        add(batches - 1, finish(middle()))
        return
    begun = begin(1)
    made = middle()
    keep_middle(made)
    keep(begun)
    lax.fori_loop(2, batches, deep_step, 0)
    sums = last()
    made = middle()
    keep_middle(made)
    add(batches - 2, sums)
    add(batches - 1, last())


def run_list(targets, sources, total, null_row, target_of, pool, acc, squares, weights, *later):
    size = 2 * squares.shape[0]
    least = 2 if later else 1
    for u in range(least * size):
        targets[total + u] = 0
        sources[total + u] = null_row
    batches = jnp.maximum(lax.div(total + (size - 1), size), least)
    run_pairs(
        batches,
        lambda i, u: targets[i * size + u],
        lambda i, u: sources[i * size + u],
        target_of,
        pool, acc, squares, weights, *later,
    )


def append(begin, end, entry, targets, sources, total):
    def step(i, total):
        j = begin + i * CHUNK
        found = [entry(j + v) for v in range(CHUNK)]
        for v, (target, source, valid) in enumerate(found):
            targets[total] = target
            sources[total] = source
            total = total + jnp.where((j + v < end) & valid, 1, 0)
        return total

    return lax.fori_loop(0, lax.shift_right_logical(end - begin + (CHUNK - 1), CHUNK.bit_length() - 1), step, total)


def append_local(tables, wanted, targets, sources, total, sent, pairs):
    at_local = table_places(pairs, sent)[1] + LOCAL

    def both(j, n):
        code = tables[0, j]
        t = lax.shift_right_logical(code, CODE.bit_length() - 1)
        u = code & (CODE - 1)
        targets[n] = t
        sources[n] = 4 * u
        targets[n + 1] = u
        sources[n + 1] = 4 * t
        return n + 2

    begin = tables[0, at_local]
    return lax.fori_loop(begin, jnp.where(wanted, tables[0, at_local + 1], begin), both, total)


def append_ghosts(tables, offsets, first, row, stride, targets, sources, total, leaves, sent, pairs):
    at_slots, at_starts = table_places(pairs, sent)
    bits = CODE.bit_length() - 1

    def slot(code, k):
        return at_slots + (((code & (CODE - 1)) - (leaves + k * sent)) & (at_starts - at_slots - 1))

    for n, k in enumerate(offsets):
        at = row + n * stride

        def mine(j, n=n, k=k, at=at):
            code = tables[0, j]
            leaf = tables[first + n, slot(code, k)]
            return lax.shift_right_logical(code, bits), at + 4 * leaf, leaf >= 0

        total = append(tables[0, at_starts + k], tables[0, at_starts + k + 1], mine, targets, sources, total)
        back = 7 - k

        def theirs(j, n=n, back=back, at=at):
            code = tables[first + n, j]
            leaf = tables[0, slot(code, back)]
            return leaf, at + 4 * lax.shift_right_logical(code, bits), leaf >= 0

        total = append(tables[first + n, at_starts + back], tables[first + n, at_starts + back + 1], theirs, targets, sources, total)
    return total


def fetch_tables(parts, staging, tables, sem):
    for n, (ref, row) in enumerate(parts):
        staging[pl.ds(n, 1), :] = ref[pl.ds(row, 1), :].astype(jnp.int32)
    copy = pltpu.make_async_copy(staging, tables, sem)
    copy.start()
    return copy


def own_kernel(own, acc, stacks, staging, tables, targets, sources, squares, weights, factor, moments, sem, *, leaves, sent, pairs, index_of):
    rows = 4 * leaves
    copy = fetch_tables([(own, rows)], staging, tables, sem)
    acc[...] = jnp.zeros_like(acc)
    for leaf in range(leaves):
        targets[leaf] = leaf
        sources[leaf] = 4 * leaf
    copy.wait()
    total = append_local(tables, index_of() == 0, targets, sources, leaves, sent, pairs)

    def target_of(leaf):
        stack = target_stack(own[pl.ds(4 * leaf, 8), :])
        stacks[leaf] = stack
        return stack

    run_list(targets, sources, total, rows, target_of, own, acc, squares, weights, factor, moments)


def forces(acc, packed, leaves):
    def part(c):
        return acc[pl.ds(c, leaves, stride=8), :] + acc[pl.ds(c + 4, leaves, stride=8), :]

    mass = packed[pl.ds(3, leaves, stride=4), :]
    norm = part(3)
    return [mass * (part(c) - packed[pl.ds(c, leaves, stride=4), :] * norm) for c in range(3)]


def sent_kernel(sub_b, corners, out, acc, staging, tables, targets, sources, squares, weights, sem, *, leaves, sent, pairs, index_of):
    rows = 4 * leaves
    stride = rows + TABLE
    odd = lax.rem(index_of(), 2)
    copy = fetch_tables([(sub_b, rows), (corners, rows), (corners, stride + rows)], staging, tables, sem)
    acc[...] = jnp.zeros_like(acc)
    copy.wait()
    offsets = (2 - 2 * odd, 7 - 2 * odd)
    total = append_ghosts(tables, offsets, 1, 0, stride, targets, sources, 0, leaves, sent, pairs)
    run_list(
        targets, sources, total, rows,
        lambda leaf: target_stack(sub_b[pl.ds(4 * leaf, 8), :]),
        corners, acc, squares, weights,
    )
    for c, force in enumerate(forces(acc, sub_b, leaves)):
        out[c] = force


def near_kernel(own, space_lower, space_upper, sub_a, sub_b, corner_a, stacks, acc_in, out, acc, pool, staging, tables, targets, sources, squares, weights, factor, moments, sem, *, leaves, sent, pairs, index_of):
    rows = 4 * leaves
    stride = rows + TABLE
    index = index_of()
    odd = lax.rem(index, 2)
    parts = [(own, 0), (space_lower, 0), (space_upper, 0), (sub_a, 0), (sub_b, 0), (corner_a, 0), (corner_a, stride)]
    copy = fetch_tables([(ref, row + rows) for ref, row in parts], staging, tables, sem)
    acc[...] = acc_in[...]
    for n, (ref, row) in enumerate(parts):
        pool[pl.ds(n * stride, stride), :] = ref[pl.ds(row, stride), :]
    copy.wait()

    total = append_local(tables, index != 0, targets, sources, 0, sent, pairs)
    offsets = (1, 6, 4 - odd, 3 + odd, 2 - 2 * odd, 7 - 2 * odd)
    total = append_ghosts(tables, offsets, 1, stride, stride, targets, sources, total, leaves, sent, pairs)
    run_list(targets, sources, total, rows, lambda leaf: stacks[leaf], pool, acc, squares, weights, factor, moments)
    for c, force in enumerate(forces(acc, own, leaves)):
        out[c] = force


def ring(size, step):
    return [(i, (i + step) % size) for i in range(size)]


def both_ways(value, axis):
    size = lax.axis_size(axis)
    lower = lax.ppermute(value, axis, ring(size, 1))
    upper = lax.ppermute(value, axis, ring(size, -1))
    return lower, upper


def swapped(value, axis, first):
    size = lax.axis_size(axis)
    pairs = [(i, (i + 1) % size) for i in range(first, size, 2)]
    return lax.ppermute(value, axis, pairs + [(j, i) for i, j in pairs])


def local(positions, masses, occupancy, export_slots, export_count, pair_list, pair_count):
    leaves, lanes = masses.shape[1:]
    sent = export_slots.shape[1]
    slots_of_pairs = pair_list.shape[2]
    rows = 4 * leaves + TABLE
    f32 = jnp.float32
    lane = lax.broadcasted_iota(jnp.int32, (1, lanes), 1)
    counts = jnp.where(lane < lanes // 2, export_count[0, 0], pair_count[0, 0])
    packed = pl.pallas_call(
        functools.partial(pack_kernel, leaves=leaves, sent=sent, slots_of_pairs=slots_of_pairs),
        out_shape=pltpu.VMEM((rows, lanes), f32),
        in_specs=[vmem()] * 6,
        out_specs=vmem(),
        name="pack",
    )(positions, masses, occupancy, export_slots, pair_list, on_chip(counts))

    def pairing(batch, deep):
        stages = [
            pltpu.VMEM((batch // 2, lanes, 2 * lanes), f32),
            pltpu.VMEM((batch // 2, 32, lanes), jnp.bfloat16),
        ]
        if deep:
            stages += [
                pltpu.VMEM((batch // 2, 2 * lanes, 2 * lanes), jnp.bfloat16),
                pltpu.VMEM((batch // 2, 32, lanes), jnp.bfloat16),
            ]
        return stages

    def lists(parts, entries, batch, deep):
        return [
            pltpu.VMEM((parts, lanes), jnp.int32),
            pltpu.SMEM((parts, lanes), jnp.int32),
            pltpu.SMEM((entries + 2 * batch + CHUNK,), jnp.int32),
            pltpu.SMEM((entries + 2 * batch + CHUNK,), jnp.int32),
            *pairing(batch, deep),
            pltpu.SemaphoreType.DMA,
        ]

    def cost(blocks):
        return pl.CostEstimate(flops=blocks * lanes * lanes * 200, transcendentals=0, bytes_accessed=rows * lanes * 4)

    accumulator = pltpu.VMEM((8 * leaves, lanes), f32)
    force = pltpu.VMEM((3, leaves, lanes), f32)
    sizes = dict(leaves=leaves, sent=sent, pairs=slots_of_pairs, index_of=functools.partial(lax.axis_index, "sub"))
    space_lower, space_upper = both_ways(packed, "space")
    sub_a = swapped(packed, "sub", 0)
    sub_b = swapped(packed, "sub", 1)
    acc, stacks = pl.pallas_call(
        functools.partial(own_kernel, **sizes),
        out_shape=(accumulator, pltpu.VMEM((leaves, STACK, lanes), jnp.bfloat16)),
        in_specs=[vmem()],
        out_specs=(vmem(), vmem()),
        scratch_shapes=lists(1, leaves + 2 * slots_of_pairs, OWN_BATCH, True),
        cost_estimate=cost(leaves),
        name="own_pairs",
    )(on_chip(packed))
    corners = jnp.concatenate([space_lower, space_upper], axis=0)
    corner_a = swapped(corners, "sub", 0)
    for_b = pl.pallas_call(
        functools.partial(sent_kernel, **sizes),
        out_shape=force,
        in_specs=[vmem()] * 2,
        out_specs=vmem(),
        scratch_shapes=[pltpu.VMEM((8 * leaves, lanes), f32)] + lists(3, 3 * slots_of_pairs, SENT_BATCH, False),
        cost_estimate=cost(slots_of_pairs),
        name="sent_pairs",
    )(*map(on_chip, (sub_b, corners)))
    from_b = swapped(for_b, "sub", 1)
    near = pl.pallas_call(
        functools.partial(near_kernel, **sizes),
        out_shape=force,
        in_specs=[vmem()] * 8,
        out_specs=vmem(),
        scratch_shapes=[pltpu.VMEM((8 * leaves, lanes), f32), pltpu.VMEM((7 * rows, lanes), f32)]
        + lists(7, 8 * slots_of_pairs, NEAR_BATCH, True),
        cost_estimate=cost(slots_of_pairs),
        name="near_pairs",
    )(*map(on_chip, (packed, space_lower, space_upper, sub_a, sub_b, corner_a, stacks, acc)))
    return (near + from_b)[:, None]


def solution(mesh):
    return jax.shard_map(
        local,
        mesh=mesh,
        in_specs=(
            P(None, "space", "sub", None),
            P("space", "sub", None),
            P("space", "sub"),
            P("space", "sub"),
            P("space", "sub"),
            P(None, "space", "sub"),
            P("space", "sub"),
        ),
        out_specs=P(None, "space", "sub", None),
        check_vma=False,
    )
```
